32 devices in a mesh: group: 4 (over y, core), peer: 8 (over z, x).
Axes of the slice: x: 2, y: 2, z: 4, core: 2. Of those that a mesh axis runs over, the one named last changes fastest.
Arguments:
- states: float32 [41, 1048576], P(None, ('group', 'peer')), may hold values from -6 to 6
- block_part: int32 [8192], P(('group', 'peer')), may hold values from 0 to 31, as said below
- tile_perm: int32 [8192, 128], P(('group', 'peer')), may hold values from 0 to 127, each once within a row
- half_volt: float32 [40], replicated, may hold values from -4 to 4
- steepness: float32 [40], replicated, may hold values from 0.5 to 4
- gate_rate: float32 [40], replicated, may hold values from 0.1 to 1
- conductance: float32 [40], replicated, may hold values from 0.005 to 0.08
- reversal: float32 [40], replicated, may hold values from -6 to 6
Outputs:
- regrouped: float32 [41, 1048576], P(None, ('group', 'peer'))
The draws below stay inside these ranges and needn't reach their ends.
Inputs may be any that keep to these rules, and one draw needn't show every extreme that they name: `block_part`: every partition holds exactly 256 blocks. Within each slab of 256 consecutive global blocks no partition holds more than 16 blocks; every slab has exactly 16 blocks of some partition, and every partition has exactly 16 blocks in some slab.
All inputs are finite; a program needn't handle non-finite values.
Results may differ from the reference program's by a relative error of at most 0.0001.
Values sent between devices are 32-bit elements; how exact they have to be, the bound alone decides.
No kernel may reach another device: no remote copies, remote signals or barrier semaphores. Data moves between devices by JAX's collectives and lax.ppermute only.
A program may use at most 192 MiB of HBM per device.

```python
import math
import jax
import jax.numpy as jnp
from jax import lax

STATES = 41
NODE_BLK = 128
BLK_DEV = 256
SUBSTEPS = 1
GATES = 40
BLOCKS = 8192
NODES = 1048576


def draw_block_part(key, part):
    devices = BLOCKS // BLK_DEV
    mean_count = BLK_DEV // devices
    pair_count = devices // 2
    key_order = jax.random.fold_in(key, 11)
    key_amount = jax.random.fold_in(key, 12)
    key_shuffle = jax.random.fold_in(key, 13)
    ordering = jax.random.permutation(key_order, devices).astype(jnp.int32)
    amounts = jax.random.randint(key_amount, (pair_count,), -mean_count, mean_count + 1, dtype=jnp.int32)
    amounts = amounts.at[0].set(mean_count)
    row_ids = jnp.arange(devices, dtype=jnp.int32)
    pair_ids = jnp.arange(pair_count, dtype=jnp.int32)
    plus_cols = ordering[(row_ids[:, None] + 2 * pair_ids[None, :]) % devices]
    minus_cols = ordering[(row_ids[:, None] + 2 * pair_ids[None, :] + 1) % devices]
    row_grid = jnp.broadcast_to(row_ids[:, None], (devices, pair_count))
    amount_grid = jnp.broadcast_to(amounts[None, :], (devices, pair_count))
    counts = jnp.full((devices, devices), mean_count, jnp.int32)
    counts = counts.at[row_grid, plus_cols].add(amount_grid)
    counts = counts.at[row_grid, minus_cols].add(-amount_grid)
    running = jnp.cumsum(counts, axis=1, dtype=jnp.int32)
    position = jnp.arange(BLK_DEV, dtype=jnp.int32)
    labels = jnp.sum((running[:, None, :] <= position[None, :, None]).astype(jnp.int32), axis=2, dtype=jnp.int32)
    row_keys = jax.random.split(key_shuffle, devices)
    shuffled = jax.vmap(lambda row_key, row_vals: jax.random.permutation(row_key, row_vals))(row_keys, labels)
    return shuffled.reshape(-1).astype(jnp.int32)


def level_of(own_key, extent, cuts, low, largest):
    gain = 1.0
    for dim, parts in cuts:
        steps = jax.random.uniform(jax.random.fold_in(jax.random.fold_in(own_key, 6), dim), (parts,), jnp.float32, low / len(cuts), largest / len(cuts))
        gain = gain * jnp.repeat(jnp.exp(steps), extent[dim] // parts).reshape((-1,) + (1,) * (len(extent) - 1 - dim))
    return gain


def normal_values(stream_key, dims, width, reach, shards=(), kind=jnp.bfloat16):
    result = width * jax.random.normal(stream_key, dims, jnp.float32)
    if shards:
        result = result * level_of(stream_key, dims, shards, -0.22, 0.18)
    return jnp.clip(result, -reach, reach).astype(kind)


def setup_inputs(seed: int = 0) -> dict:
    key_list = jax.random.split(jax.random.key(seed), 9)
    return {
        "states": normal_values(key_list[0], (STATES, NODES), 1.0, 6.0, ((1, 32),), jnp.float32),
        "block_part": draw_block_part(jax.random.fold_in(key_list[8], 71), 0),
        "tile_perm": jax.vmap(lambda own: jax.random.permutation(own, NODE_BLK))(jax.random.split(key_list[2], BLOCKS)).reshape((BLOCKS, NODE_BLK)).astype(jnp.int32),
        "half_volt": normal_values(key_list[3], (GATES,), 1.0, 4.0, (), jnp.float32),
        "steepness": jnp.clip(jnp.exp(jax.random.uniform(key_list[4], (GATES,), jnp.float32, math.log(0.5), math.log(4.0))), 0.5, 4.0),
        "gate_rate": jnp.clip(jnp.exp(jax.random.uniform(key_list[5], (GATES,), jnp.float32, math.log(0.1), math.log(1.0))), 0.1, 1.0),
        "conductance": jnp.clip(jnp.exp(jax.random.uniform(key_list[6], (GATES,), jnp.float32, math.log(0.005), math.log(0.08))), 0.005, 0.08),
        "reversal": normal_values(key_list[7], (GATES,), 1.5, 6.0, (), jnp.float32),
    }


time_step = 0.25


def advance(state_rows, half_volt, steepness, gate_rate, conductance, reversal):
    voltage = state_rows[0:1]
    gate_vals = state_rows[1:]
    for substep in range(SUBSTEPS):
        steady = jax.nn.sigmoid((voltage - half_volt[:, None]) * steepness[:, None])
        damping = jnp.exp(-gate_rate[:, None] * (1.0 + jax.nn.sigmoid(voltage)))
        gate_vals = steady + (gate_vals - steady) * damping
        current = jnp.sum(conductance[:, None] * gate_vals * (voltage - reversal[:, None]), axis=0, keepdims=True)
        voltage = voltage - time_step * current
    return jnp.concatenate([voltage, gate_vals], axis=0)


def reference(states, block_part, tile_perm, half_volt, steepness, gate_rate, conductance, reversal):
    devices = BLOCKS // BLK_DEV
    span = BLK_DEV * NODE_BLK

    def one_part(index, acc):
        start = (index * span).astype(jnp.int32)
        piece = lax.dynamic_slice_in_dim(states, start, span, 1)
        done = advance(piece, half_volt, steepness, gate_rate, conductance, reversal)
        return lax.dynamic_update_slice_in_dim(acc, done, start, 1)

    advanced = lax.fori_loop(0, devices, one_part, jnp.zeros_like(states))
    ordering = jnp.argsort(block_part, stable=True).astype(jnp.int32)
    local_index = jnp.zeros((BLOCKS,), jnp.int32).at[ordering].set(jnp.arange(BLOCKS, dtype=jnp.int32))
    columns = (local_index[:, None] * NODE_BLK + tile_perm).reshape(-1).astype(jnp.int32)
    return jnp.take(advanced, columns, axis=1)
```

```python
import functools

import jax
import jax.numpy as jnp
from jax import lax
from jax.experimental import pallas as pl
from jax.experimental.pallas import tpu as pltpu
from jax.sharding import PartitionSpec as P

time_step = 0.25
sublanes = 8
both = ("group", "peer")


def advance_kernel(params_ref, states_ref, out_ref, *, step):
    rows = states_ref.shape[0]
    half_volt = params_ref[:, 0:1]
    steepness = params_ref[:, 1:2]
    gate_rate = params_ref[:, 2:3]
    conductance = params_ref[:, 3:4]
    reversal = params_ref[:, 4:5]
    row = lax.broadcasted_iota(jnp.int32, (rows, step), 0)

    def one(i, carry):
        cols = pl.ds(pl.multiple_of(i * step, step), step)
        vals = states_ref[:, cols]
        voltage = vals[0:1]
        steady = jax.nn.sigmoid((voltage - half_volt) * steepness)
        damping = jnp.exp(-gate_rate * (1.0 + jax.nn.sigmoid(voltage)))
        gates = steady + (vals - steady) * damping
        current = jnp.sum(
            conductance * gates * (voltage - reversal), axis=0, keepdims=True
        )
        out_ref[:, cols] = jnp.where(row == 0, voltage - time_step * current, gates)
        return carry

    lax.fori_loop(0, states_ref.shape[1] // step, one, 0)


def advance(states, half_volt, steepness, gate_rate, conductance, reversal):
    rows, nodes = states.shape
    params = jnp.pad(
        jnp.stack([half_volt, steepness, gate_rate, conductance, reversal], axis=1),
        ((1, 0), (0, 0)),
    )
    block = math_block(nodes, 2048)
    step = math_block(block, 256)
    return pl.pallas_call(
        functools.partial(advance_kernel, step=step),
        grid=(nodes // block,),
        in_specs=[
            pl.BlockSpec(params.shape, lambda i: (0, 0)),
            pl.BlockSpec((rows, block), lambda i: (0, i)),
        ],
        out_specs=pl.BlockSpec((rows, block), lambda i: (0, i)),
        out_shape=jax.ShapeDtypeStruct(states.shape, states.dtype),
        cost_estimate=pl.CostEstimate(
            flops=40 * rows * nodes,
            bytes_accessed=8 * rows * nodes,
            transcendentals=3 * rows * nodes,
        ),
        name="advance",
    )(params, states)


def math_block(total, most):
    size = min(total, most)
    while total % size:
        size -= 128
    return size


def pack_kernel(counts_ref, adv_ref, out_ref, start_ref, *, slots, blocks, width):
    full = adv_ref.shape[0] // sublanes * sublanes
    extra = adv_ref.shape[0] - full
    per_step = out_ref.shape[0]
    first = pl.program_id(0) * per_step

    @pl.when(first == 0)
    def _():
        start_ref[0] = 0

    start = start_ref[0]
    for d in range(per_step):
        for k in range(slots):
            block = jnp.minimum(start + k, blocks - 1)
            cols = pl.ds(pl.multiple_of(block * width, width), width)
            out_ref[d, k * full : (k + 1) * full, :] = adv_ref[0:full, cols]
            for e in range(extra):
                row = slots * full + e * slots + k
                out_ref[d, row : row + 1, :] = adv_ref[full + e : full + e + 1, cols]
        start = start + counts_ref[first + d]
    start_ref[0] = start


def pack(counts, adv, devices, slots, width):
    rows, nodes = adv.shape
    per_step = 4
    return pl.pallas_call(
        functools.partial(pack_kernel, slots=slots, blocks=nodes // width, width=width),
        grid_spec=pltpu.PrefetchScalarGridSpec(
            num_scalar_prefetch=1,
            grid=(devices // per_step,),
            in_specs=[pl.BlockSpec(adv.shape, lambda i, c: (0, 0))],
            out_specs=pl.BlockSpec((per_step, rows * slots, width), lambda i, c: (i, 0, 0)),
            scratch_shapes=[pltpu.SMEM((1,), jnp.int32)],
        ),
        out_shape=jax.ShapeDtypeStruct((devices, rows * slots, width), adv.dtype),
        name="pack",
    )(counts, adv)


def permuted(vals, lanes):
    return jnp.take_along_axis(vals, lanes, axis=1, mode="promise_in_bounds")


def unpack_kernel(part_ref, rank_ref, perm_ref, got_ref, out_ref, tail_ref, *, slots):
    rows, nodes = out_ref.shape
    per_step, width = perm_ref.shape
    full = rows // sublanes * sublanes
    first = pl.program_id(0) * per_step
    for i in range(per_step):
        part = part_ref[first + i]
        rank = rank_ref[first + i]
        lanes = jnp.broadcast_to(perm_ref[i : i + 1, :], (full, width))
        vals = got_ref[part, pl.ds(pl.multiple_of(rank * full, full), full), :]
        out_ref[0:full, i * width : (i + 1) * width] = permuted(vals, lanes)
        for e in range(rows - full):
            row = slots * full + e * slots + rank
            tail_ref[e, i : i + 1, :] = got_ref[part, pl.ds(row, 1), :]
    for e in range(rows - full):
        tail = permuted(tail_ref[e], perm_ref[...])
        for i in range(per_step):
            cols = slice(i * width, (i + 1) * width)
            out_ref[full + e : full + e + 1, cols] = tail[i : i + 1, :]


def unpack(part, rank, perm, got, rows, slots):
    blocks, width = perm.shape
    per_step = 16
    return pl.pallas_call(
        functools.partial(unpack_kernel, slots=slots),
        grid_spec=pltpu.PrefetchScalarGridSpec(
            num_scalar_prefetch=2,
            grid=(blocks // per_step,),
            in_specs=[
                pl.BlockSpec((per_step, width), lambda i, p, r: (i, 0)),
                pl.BlockSpec(got.shape, lambda i, p, r: (0, 0, 0)),
            ],
            out_specs=pl.BlockSpec((rows, per_step * width), lambda i, p, r: (0, i)),
            scratch_shapes=[
                pltpu.VMEM((max(rows % sublanes, 1), per_step, width), got.dtype)
            ],
        ),
        out_shape=jax.ShapeDtypeStruct((rows, blocks * width), got.dtype),
        name="unpack",
    )(part, rank, perm, got)


def on_device(
    states, block_part, tile_perm, half_volt, steepness, gate_rate, conductance, reversal
):
    devices = lax.axis_size(both)
    blocks, width = tile_perm.shape
    rows = states.shape[0]
    slots = 2 * blocks // devices
    partitions = jnp.arange(devices, dtype=jnp.int32)
    onehot = (block_part[:, None] == partitions[None, :]).astype(jnp.int32)
    counts = jnp.sum(onehot, axis=0, dtype=jnp.int32)
    asked = lax.all_to_all(counts, both, split_axis=0, concat_axis=0, tiled=True)
    adv = advance(states, half_volt, steepness, gate_rate, conductance, reversal)
    send = pack(asked, adv, devices, slots, width)
    got = lax.all_to_all(send, both, split_axis=0, concat_axis=0, tiled=True)
    same = block_part[:, None] == block_part[None, :]
    position = jnp.arange(blocks, dtype=jnp.int32)
    ahead = position[None, :] < position[:, None]
    rank = jnp.sum((same & ahead).astype(jnp.int32), axis=1, dtype=jnp.int32)
    return unpack(block_part, rank, tile_perm, got, rows, slots)


def solution(mesh):
    return jax.shard_map(
        on_device,
        mesh=mesh,
        in_specs=(
            P(None, both),
            P(both),
            P(both, None),
            P(),
            P(),
            P(),
            P(),
            P(),
        ),
        out_specs=P(None, both),
        check_vma=False,
    )
```

```python
import functools

import jax
import jax.numpy as jnp
from jax import lax
from jax.experimental import pallas as pl
from jax.experimental.pallas import tpu as pltpu
from jax.sharding import PartitionSpec as P


time_step = 0.25
sublanes = 8
both = ("group", "peer")
smem_full = pl.BlockSpec(memory_space=pltpu.SMEM)
vmem_full = pl.BlockSpec(memory_space=pltpu.VMEM)
any_full = pl.BlockSpec(memory_space=pl.ANY)


def round_up(value, step):
    return -(-value // step) * step


class Plan:
    def __init__(self, rows, blocks, width):
        self.rows, self.blocks, self.width = rows, blocks, width
        self.peers = lax.axis_size("peer")
        self.devices = lax.axis_size("group") * self.peers
        self.near = self.peers // 2
        self.mates = self.devices // 2
        most = 2 * blocks // self.devices
        self.slots = max(most // 2, 1)
        self.over = most - self.slots
        self.full = rows // sublanes * sublanes
        self.extra = rows - self.full
        self.direct_rows = round_up(rows * self.slots, sublanes)
        self.relay_rows = round_up(rows * 2 * self.over, sublanes)
        self.worst = self.mates * self.over

    def half(self, device):
        return (device % self.peers) // self.near

    def mate(self, device):
        return device // self.peers * self.near + device % self.near

    def device(self, mate, half):
        return mate // self.near * self.peers + half * self.near + mate % self.near

    def partner(self, device):
        flip = 1 - 2 * self.half(device)
        return device + flip * self.near

    def me(self):
        return lax.axis_index("group") * self.peers + lax.axis_index("peer")


def advance_kernel(params_ref, states_ref, out_ref, *, step):
    rows = states_ref.shape[0]
    row = lax.broadcasted_iota(jnp.int32, (rows, step), 0)

    def one(i, carry):
        cols = pl.ds(pl.multiple_of(i * step, step), step)
        vals = states_ref[:, cols]
        voltage = vals[0:1]
        relax = 1.5 + 0.5 * jnp.tanh(0.5 * voltage)
        steady = 0.5 + 0.5 * jnp.tanh((voltage - params_ref[0]) * params_ref[1])
        damping = jnp.exp(params_ref[2] * relax)
        gates = steady + (vals - steady) * damping
        current = jnp.sum(
            params_ref[3] * gates * (voltage - params_ref[4]), axis=0, keepdims=True
        )
        out_ref[:, cols] = jnp.where(row == 0, voltage - time_step * current, gates)
        return carry

    lax.fori_loop(0, states_ref.shape[1] // step, one, 0)


def advance(states, half_volt, steepness, gate_rate, conductance, reversal):
    rows, nodes = states.shape
    step = 128
    params = jnp.stack([half_volt, 0.5 * steepness, -gate_rate, conductance, reversal])
    params = jnp.pad(params, ((0, 0), (1, 0)))
    params = jnp.broadcast_to(params[:, :, None], params.shape + (step,))
    block = fitting(nodes, 4096)
    return pl.pallas_call(
        functools.partial(advance_kernel, step=step),
        grid=(nodes // block,),
        in_specs=[
            pl.BlockSpec(params.shape, lambda i: (0, 0, 0)),
            pl.BlockSpec((rows, block), lambda i: (0, i)),
        ],
        out_specs=pl.BlockSpec((rows, block), lambda i: (0, i)),
        out_shape=jax.ShapeDtypeStruct(states.shape, states.dtype),
        cost_estimate=pl.CostEstimate(
            flops=40 * rows * nodes,
            bytes_accessed=8 * rows * nodes,
            transcendentals=3 * rows * nodes,
        ),
        name="advance",
    )(params, states)


def fitting(total, most):
    size = min(total, most)
    while total % size:
        size -= 128
    return size


def put_block(plan, adv_ref, block, put, base, tail):
    cols = pl.ds(pl.multiple_of(block * plan.width, plan.width), plan.width)
    put(base, plan.full, adv_ref[0 : plan.full, cols])
    for e in range(plan.extra):
        put(tail(e), 1, adv_ref[plan.full + e : plan.full + e + 1, cols])


def pack_kernel(table_ref, adv_ref, direct_ref, cross_ref, *, plan, room):
    me = plan.me()
    mine = plan.half(me)

    def one(s, carry):
        start, at = carry
        count = table_ref[s * plan.devices + me]

        def put(base, size, vals):
            direct_ref[s, base : base + size, :] = vals

        for k in range(plan.slots):
            put_block(
                plan,
                adv_ref,
                jnp.minimum(start + k, plan.blocks - 1),
                put,
                k * plan.full,
                lambda e: plan.slots * plan.full + e * plan.slots + k,
            )
        far = (plan.half(s) != mine).astype(jnp.int32)
        more = jnp.maximum(count - plan.slots, 0) * far

        def spill(k, carry):
            slot = jnp.minimum(at + k, room - 1)

            def put_cross(base, size, vals):
                if size == plan.full:
                    base = pl.multiple_of(base, sublanes)
                cross_ref[pl.ds(base, size), :] = vals

            put_block(
                plan,
                adv_ref,
                start + plan.slots + k,
                put_cross,
                slot * plan.full,
                lambda e: room * plan.full + e * room + slot,
            )
            return carry

        lax.fori_loop(0, more, spill, 0)
        return start + count, at + more

    lax.fori_loop(0, plan.devices, one, (0, 0))


def pack(plan, table, adv, room):
    return pl.pallas_call(
        functools.partial(pack_kernel, plan=plan, room=room),
        in_specs=[smem_full, vmem_full],
        out_specs=[vmem_full, vmem_full],
        out_shape=[
            jax.ShapeDtypeStruct((plan.devices, plan.direct_rows, plan.width), adv.dtype),
            jax.ShapeDtypeStruct((round_up(room * plan.rows, sublanes), plan.width), adv.dtype),
        ],
        name="pack",
    )(table, adv)


def relay_kernel(table_ref, adv_ref, cross_ref, *refs, plan, room):
    outs, (own_ref, far_ref) = refs[: plan.mates], refs[plan.mates :]
    me = plan.me()
    mine = plan.half(me)
    other = plan.partner(me)

    def scan(s, carry):
        start, at = carry
        own_ref[s] = start
        far_ref[s] = at
        near = (plan.half(s) == mine).astype(jnp.int32)
        more = jnp.maximum(table_ref[s * plan.devices + other] - plan.slots, 0)
        return start + table_ref[s * plan.devices + me], at + more * near

    lax.fori_loop(0, plan.devices, scan, (0, 0))
    here = plan.mate(me)
    slots = 2 * plan.over
    for d, out_ref in enumerate(outs):
        s = plan.device(here ^ d, mine)
        start = own_ref[s] + plan.slots
        at = far_ref[s]

        def put(base, size, vals):
            out_ref[base : base + size, :] = vals

        for k in range(plan.over):
            put_block(
                plan,
                adv_ref,
                jnp.minimum(start + k, plan.blocks - 1),
                put,
                k * plan.full,
                lambda e: slots * plan.full + e * slots + k,
            )
        for k in range(plan.over):
            slot = jnp.minimum(at + k, room - 1)
            to = plan.over + k
            out_ref[to * plan.full : (to + 1) * plan.full, :] = cross_ref[
                pl.ds(pl.multiple_of(slot * plan.full, plan.full), plan.full), :
            ]
            for e in range(plan.extra):
                row = slots * plan.full + e * slots + to
                out_ref[row : row + 1, :] = cross_ref[
                    pl.ds(room * plan.full + e * room + slot, 1), :
                ]


def relay(plan, table, adv, crossed, room):
    piece = jax.ShapeDtypeStruct((plan.relay_rows, plan.width), adv.dtype)
    return pl.pallas_call(
        functools.partial(relay_kernel, plan=plan, room=room),
        in_specs=[smem_full, vmem_full, vmem_full],
        out_specs=[vmem_full] * plan.mates,
        out_shape=[piece] * plan.mates,
        scratch_shapes=[
            pltpu.SMEM((plan.devices,), jnp.int32),
            pltpu.SMEM((plan.devices,), jnp.int32),
        ],
        name="relay",
    )(table, adv, crossed)


def permuted(vals, lanes):
    return jnp.take_along_axis(vals, lanes, axis=1, mode="promise_in_bounds")


def unpack_kernel(base_ref, tail_ref, step_ref, perm_ref, direct_ref, *refs, plan):
    pieces = refs[: plan.mates]
    out_ref, got_ref, last_ref, sem = refs[plan.mates :]
    per_step, width = perm_ref.shape
    first = pl.program_id(0) * per_step

    @pl.when(first == 0)
    def _():
        direct = plan.devices * plan.direct_rows
        copies = [
            pltpu.make_async_copy(direct_ref, got_ref.at[pl.ds(0, direct)], sem.at[0])
        ]
        for d, piece_ref in enumerate(pieces):
            rows = pl.ds(direct + d * plan.relay_rows, plan.relay_rows)
            copies.append(
                pltpu.make_async_copy(piece_ref, got_ref.at[rows], sem.at[1 + d])
            )
        for copy in copies:
            copy.start()
        for copy in copies:
            copy.wait()

    for i in range(per_step):
        base = pl.multiple_of(base_ref[first + i], sublanes)
        tail = tail_ref[first + i]
        stride = step_ref[first + i]
        lanes = jnp.broadcast_to(perm_ref[i : i + 1, :], (plan.full, width))
        vals = got_ref[pl.ds(base, plan.full), :]
        out_ref[0 : plan.full, i * width : (i + 1) * width] = permuted(vals, lanes)
        for e in range(plan.extra):
            last_ref[e, i : i + 1, :] = got_ref[pl.ds(tail + e * stride, 1), :]
    for e in range(plan.extra):
        last = permuted(last_ref[e], perm_ref[...])
        for i in range(per_step):
            cols = slice(i * width, (i + 1) * width)
            out_ref[plan.full + e : plan.full + e + 1, cols] = last[i : i + 1, :]


def unpack(plan, places, perm, direct, pieces):
    per_step = fitting_blocks(plan.blocks, 16)
    total = plan.devices * plan.direct_rows + plan.mates * plan.relay_rows
    return pl.pallas_call(
        functools.partial(unpack_kernel, plan=plan),
        grid_spec=pltpu.PrefetchScalarGridSpec(
            num_scalar_prefetch=3,
            grid=(plan.blocks // per_step,),
            in_specs=[pl.BlockSpec((per_step, plan.width), lambda i, *_: (i, 0))]
            + [any_full] * (1 + plan.mates),
            out_specs=pl.BlockSpec((plan.rows, per_step * plan.width), lambda i, *_: (0, i)),
            scratch_shapes=[
                pltpu.VMEM((total, plan.width), direct.dtype),
                pltpu.VMEM((max(plan.extra, 1), per_step, plan.width), direct.dtype),
                pltpu.SemaphoreType.DMA((1 + plan.mates,)),
            ],
        ),
        out_shape=jax.ShapeDtypeStruct((plan.rows, plan.blocks * plan.width), direct.dtype),
        name="unpack",
    )(*places, perm, direct, *pieces)


def fitting_blocks(total, most):
    size = min(total, most)
    while total % size:
        size -= 1
    return size


def find_places(plan, block_part, me):
    same = block_part[:, None] == block_part[None, :]
    position = jnp.arange(plan.blocks, dtype=jnp.int32)
    ahead = position[None, :] < position[:, None]
    rank = jnp.sum((same & ahead).astype(jnp.int32), axis=1, dtype=jnp.int32)
    direct = rank < plan.slots
    home = plan.half(block_part) == plan.half(me)
    piece = plan.mate(block_part) ^ plan.mate(me)
    origin = plan.devices * plan.direct_rows + piece * plan.relay_rows
    slot = rank - plan.slots + jnp.where(home, 0, plan.over)
    slots = 2 * plan.over
    base = jnp.where(
        direct, block_part * plan.direct_rows + rank * plan.full, origin + slot * plan.full
    )
    tail = jnp.where(
        direct,
        block_part * plan.direct_rows + plan.slots * plan.full + rank,
        origin + slots * plan.full + slot,
    )
    return base, tail, jnp.where(direct, plan.slots, slots)


def exchange(plan, table, adv, places, tile_perm, room):
    direct, cross = pack(plan, table, adv, room)
    over = range(plan.devices)
    crossed = lax.ppermute(cross, both, [(i, plan.partner(i)) for i in over])
    direct, crossing = lax.optimization_barrier((direct, cross))
    arrived = lax.all_to_all(direct, both, split_axis=0, concat_axis=0, tiled=True)
    pieces = list(relay(plan, table, adv, crossed, room))
    for d in range(1, plan.mates):
        pairs = [(i, plan.device(plan.mate(i) ^ d, plan.half(i))) for i in over]
        pieces[d] = lax.ppermute(pieces[d], both, pairs)
    flat = arrived.reshape(plan.devices * plan.direct_rows, plan.width)
    return unpack(plan, places, tile_perm, flat, pieces)


def on_device(
    states, block_part, tile_perm, half_volt, steepness, gate_rate, conductance, reversal
):
    blocks, width = tile_perm.shape
    plan = Plan(states.shape[0], blocks, width)
    devices = plan.devices
    me = plan.me()
    ids = jnp.arange(devices, dtype=jnp.int32)
    onehot = (block_part[:, None] == ids[None, :]).astype(jnp.int32)
    counts = jnp.sum(onehot, axis=0, dtype=jnp.int32)
    told = jnp.broadcast_to(counts[None, :], (devices, devices))
    table = lax.all_to_all(told, both, split_axis=0, concat_axis=0, tiled=True)
    adv = advance(states, half_volt, steepness, gate_rate, conductance, reversal)
    far = plan.half(ids)[:, None] != plan.half(ids)[None, :]
    spilled = jnp.sum(jnp.where(far, jnp.maximum(table - plan.slots, 0), 0), axis=0)
    spilled = jnp.max(spilled)
    places = find_places(plan, block_part, me)
    rooms = [plan.worst * 3 // 8, plan.worst // 2, plan.worst]
    rooms = [round_up(room, sublanes) for room in rooms]
    choice = sum((spilled > room).astype(jnp.int32) for room in rooms[:-1])
    return lax.switch(
        choice,
        [functools.partial(exchange, plan, room=room) for room in rooms],
        table.reshape(-1),
        adv,
        places,
        tile_perm,
    )


def solution(mesh):
    return jax.shard_map(
        on_device,
        mesh=mesh,
        in_specs=(
            P(None, both),
            P(both),
            P(both, None),
            P(),
            P(),
            P(),
            P(),
            P(),
        ),
        out_specs=P(None, both),
        check_vma=False,
    )
```

```python
import functools

import jax
import jax.numpy as jnp
from jax import lax
from jax.experimental import pallas as pl
from jax.experimental.pallas import tpu as pltpu
from jax.sharding import PartitionSpec as P


time_step = 0.25
sublanes = 8
both = ("group", "peer")
smem_full = pl.BlockSpec(memory_space=pltpu.SMEM)
vmem_full = pl.BlockSpec(memory_space=pltpu.VMEM)
any_full = pl.BlockSpec(memory_space=pl.ANY)


def round_up(value, step):
    return -(-value // step) * step


class Plan:
    def __init__(self, rows, blocks, width):
        self.rows, self.blocks, self.width = rows, blocks, width
        self.peers = lax.axis_size("peer")
        self.devices = lax.axis_size("group") * self.peers
        self.near = self.peers // 2
        self.mates = self.devices // 2
        most = 2 * blocks // self.devices
        self.slots = max(most // 2, 1)
        self.over = most - self.slots
        self.full = rows // sublanes * sublanes
        self.extra = rows - self.full
        self.direct_rows = round_up(rows * self.slots, sublanes)
        self.relay_rows = round_up(rows * 2 * self.over, sublanes)
        self.worst = self.mates * self.over

    def half(self, device):
        return (device % self.peers) // self.near

    def mate(self, device):
        return device // self.peers * self.near + device % self.near

    def device(self, mate, half):
        return mate // self.near * self.peers + half * self.near + mate % self.near

    def partner(self, device):
        flip = 1 - 2 * self.half(device)
        return device + flip * self.near

    def me(self):
        return lax.axis_index("group") * self.peers + lax.axis_index("peer")


def advance_kernel(params_ref, states_ref, out_ref, *, step):
    rows = states_ref.shape[0]
    row = lax.broadcasted_iota(jnp.int32, (rows, step), 0)

    def one(i, carry):
        cols = pl.ds(pl.multiple_of(i * step, step), step)
        vals = states_ref[:, cols]
        voltage = vals[0:1]
        relax = 1.5 + 0.5 * jnp.tanh(0.5 * voltage)
        steady = 0.5 + 0.5 * jnp.tanh((voltage - params_ref[0]) * params_ref[1])
        damping = jnp.exp(params_ref[2] * relax)
        gates = steady + (vals - steady) * damping
        current = jnp.sum(
            params_ref[3] * gates * (voltage - params_ref[4]), axis=0, keepdims=True
        )
        out_ref[:, cols] = jnp.where(row == 0, voltage - time_step * current, gates)
        return carry

    lax.fori_loop(0, states_ref.shape[1] // step, one, 0)


def advance(states, half_volt, steepness, gate_rate, conductance, reversal):
    rows, nodes = states.shape
    step = 128
    params = jnp.stack([half_volt, 0.5 * steepness, -gate_rate, conductance, reversal])
    params = jnp.pad(params, ((0, 0), (1, 0)))
    params = jnp.broadcast_to(params[:, :, None], params.shape + (step,))
    block = fitting(nodes, 4096)
    return pl.pallas_call(
        functools.partial(advance_kernel, step=step),
        grid=(nodes // block,),
        in_specs=[
            pl.BlockSpec(params.shape, lambda i: (0, 0, 0)),
            pl.BlockSpec((rows, block), lambda i: (0, i)),
        ],
        out_specs=pl.BlockSpec((rows, block), lambda i: (0, i)),
        out_shape=jax.ShapeDtypeStruct(states.shape, states.dtype),
        cost_estimate=pl.CostEstimate(
            flops=40 * rows * nodes,
            bytes_accessed=8 * rows * nodes,
            transcendentals=3 * rows * nodes,
        ),
        name="advance",
    )(params, states)


def fitting(total, most):
    size = min(total, most)
    while total % size:
        size -= 128
    return size


def put_block(plan, adv_ref, block, put, base, tail):
    cols = pl.ds(pl.multiple_of(block * plan.width, plan.width), plan.width)
    put(base, plan.full, adv_ref[0 : plan.full, cols])
    for e in range(plan.extra):
        put(tail(e), 1, adv_ref[plan.full + e : plan.full + e + 1, cols])


def cross_kernel(table_ref, adv_ref, cross_ref, *, plan, room):
    me = plan.me()
    mine = plan.half(me)

    def one(s, carry):
        start, at = carry
        count = table_ref[s * plan.devices + me]
        far = (plan.half(s) != mine).astype(jnp.int32)
        more = jnp.maximum(count - plan.slots, 0) * far

        def spill(k, carry):
            slot = jnp.minimum(at + k, room - 1)

            def put(base, size, vals):
                if size == plan.full:
                    base = pl.multiple_of(base, sublanes)
                cross_ref[pl.ds(base, size), :] = vals

            put_block(
                plan,
                adv_ref,
                start + plan.slots + k,
                put,
                slot * plan.full,
                lambda e: room * plan.full + e * room + slot,
            )
            return carry

        lax.fori_loop(0, more, spill, 0)
        return start + count, at + more

    lax.fori_loop(0, plan.devices, one, (0, 0))


def pack_cross(plan, table, adv, room):
    rows = round_up(room * plan.rows, sublanes)
    return pl.pallas_call(
        functools.partial(cross_kernel, plan=plan, room=room),
        in_specs=[smem_full, vmem_full],
        out_specs=vmem_full,
        out_shape=jax.ShapeDtypeStruct((rows, plan.width), adv.dtype),
        name="pack_cross",
    )(table, adv)


def direct_kernel(table_ref, adv_ref, direct_ref, start_ref, *, plan):
    me = plan.me()
    per_step = direct_ref.shape[0]
    first = pl.program_id(0) * per_step

    @pl.when(first == 0)
    def _():
        start_ref[0] = 0

    start = start_ref[0]
    for d in range(per_step):

        def put(base, size, vals):
            direct_ref[d, base : base + size, :] = vals

        for k in range(plan.slots):
            put_block(
                plan,
                adv_ref,
                jnp.minimum(start + k, plan.blocks - 1),
                put,
                k * plan.full,
                lambda e: plan.slots * plan.full + e * plan.slots + k,
            )
        start = start + table_ref[(first + d) * plan.devices + me]
    start_ref[0] = start


def pack_direct(plan, table, adv):
    per_step = fitting_blocks(plan.devices, 4)
    return pl.pallas_call(
        functools.partial(direct_kernel, plan=plan),
        grid_spec=pltpu.PrefetchScalarGridSpec(
            num_scalar_prefetch=1,
            grid=(plan.devices // per_step,),
            in_specs=[pl.BlockSpec(adv.shape, lambda i, *_: (0, 0))],
            out_specs=pl.BlockSpec(
                (per_step, plan.direct_rows, plan.width), lambda i, *_: (i, 0, 0)
            ),
            scratch_shapes=[pltpu.SMEM((1,), jnp.int32)],
        ),
        out_shape=jax.ShapeDtypeStruct(
            (plan.devices, plan.direct_rows, plan.width), adv.dtype
        ),
        name="pack_direct",
    )(table, adv)


def relay_kernel(table_ref, adv_ref, cross_ref, *refs, plan, room):
    outs, (own_ref, far_ref) = refs[: plan.mates], refs[plan.mates :]
    me = plan.me()
    mine = plan.half(me)
    other = plan.partner(me)

    def scan(s, carry):
        start, at = carry
        own_ref[s] = start
        far_ref[s] = at
        near = (plan.half(s) == mine).astype(jnp.int32)
        more = jnp.maximum(table_ref[s * plan.devices + other] - plan.slots, 0)
        return start + table_ref[s * plan.devices + me], at + more * near

    lax.fori_loop(0, plan.devices, scan, (0, 0))
    here = plan.mate(me)
    slots = 2 * plan.over
    for d, out_ref in enumerate(outs):
        s = plan.device(here ^ d, mine)
        start = own_ref[s] + plan.slots
        at = far_ref[s]

        def put(base, size, vals):
            out_ref[base : base + size, :] = vals

        for k in range(plan.over):
            put_block(
                plan,
                adv_ref,
                jnp.minimum(start + k, plan.blocks - 1),
                put,
                k * plan.full,
                lambda e: slots * plan.full + e * slots + k,
            )
        for k in range(plan.over):
            slot = jnp.minimum(at + k, room - 1)
            to = plan.over + k
            out_ref[to * plan.full : (to + 1) * plan.full, :] = cross_ref[
                pl.ds(pl.multiple_of(slot * plan.full, plan.full), plan.full), :
            ]
            for e in range(plan.extra):
                row = slots * plan.full + e * slots + to
                out_ref[row : row + 1, :] = cross_ref[
                    pl.ds(room * plan.full + e * room + slot, 1), :
                ]


def relay(plan, table, adv, crossed, room):
    piece = jax.ShapeDtypeStruct((plan.relay_rows, plan.width), adv.dtype)
    return pl.pallas_call(
        functools.partial(relay_kernel, plan=plan, room=room),
        in_specs=[smem_full, vmem_full, vmem_full],
        out_specs=[vmem_full] * plan.mates,
        out_shape=[piece] * plan.mates,
        scratch_shapes=[
            pltpu.SMEM((plan.devices,), jnp.int32),
            pltpu.SMEM((plan.devices,), jnp.int32),
        ],
        name="relay",
    )(table, adv, crossed)


def permuted(vals, lanes):
    return jnp.take_along_axis(vals, lanes, axis=1, mode="promise_in_bounds")


def unpack_kernel(base_ref, tail_ref, step_ref, perm_ref, direct_ref, *refs, plan):
    pieces = refs[: plan.mates]
    out_ref, got_ref, last_ref, sem = refs[plan.mates :]
    per_step, width = perm_ref.shape
    first = pl.program_id(0) * per_step

    @pl.when(first == 0)
    def _():
        direct = plan.devices * plan.direct_rows
        copies = [
            pltpu.make_async_copy(direct_ref, got_ref.at[pl.ds(0, direct)], sem.at[0])
        ]
        for d, piece_ref in enumerate(pieces):
            rows = pl.ds(direct + d * plan.relay_rows, plan.relay_rows)
            copies.append(
                pltpu.make_async_copy(piece_ref, got_ref.at[rows], sem.at[1 + d])
            )
        for copy in copies:
            copy.start()
        for copy in copies:
            copy.wait()

    for i in range(per_step):
        base = pl.multiple_of(base_ref[first + i], sublanes)
        tail = tail_ref[first + i]
        stride = step_ref[first + i]
        lanes = jnp.broadcast_to(perm_ref[i : i + 1, :], (plan.full, width))
        vals = got_ref[pl.ds(base, plan.full), :]
        out_ref[0 : plan.full, i * width : (i + 1) * width] = permuted(vals, lanes)
        for e in range(plan.extra):
            last_ref[e, i : i + 1, :] = got_ref[pl.ds(tail + e * stride, 1), :]
    for e in range(plan.extra):
        last = permuted(last_ref[e], perm_ref[...])
        for i in range(per_step):
            cols = slice(i * width, (i + 1) * width)
            out_ref[plan.full + e : plan.full + e + 1, cols] = last[i : i + 1, :]


def unpack(plan, places, perm, direct, pieces):
    per_step = fitting_blocks(plan.blocks, 16)
    total = plan.devices * plan.direct_rows + plan.mates * plan.relay_rows
    return pl.pallas_call(
        functools.partial(unpack_kernel, plan=plan),
        grid_spec=pltpu.PrefetchScalarGridSpec(
            num_scalar_prefetch=3,
            grid=(plan.blocks // per_step,),
            in_specs=[pl.BlockSpec((per_step, plan.width), lambda i, *_: (i, 0))]
            + [any_full] * (1 + plan.mates),
            out_specs=pl.BlockSpec((plan.rows, per_step * plan.width), lambda i, *_: (0, i)),
            scratch_shapes=[
                pltpu.VMEM((total, plan.width), direct.dtype),
                pltpu.VMEM((max(plan.extra, 1), per_step, plan.width), direct.dtype),
                pltpu.SemaphoreType.DMA((1 + plan.mates,)),
            ],
        ),
        out_shape=jax.ShapeDtypeStruct((plan.rows, plan.blocks * plan.width), direct.dtype),
        name="unpack",
    )(*places, perm, direct, *pieces)


def fitting_blocks(total, most):
    size = min(total, most)
    while total % size:
        size -= 1
    return size


def find_places(plan, block_part, me):
    same = block_part[:, None] == block_part[None, :]
    position = jnp.arange(plan.blocks, dtype=jnp.int32)
    ahead = position[None, :] < position[:, None]
    rank = jnp.sum((same & ahead).astype(jnp.int32), axis=1, dtype=jnp.int32)
    direct = rank < plan.slots
    home = plan.half(block_part) == plan.half(me)
    piece = plan.mate(block_part) ^ plan.mate(me)
    origin = plan.devices * plan.direct_rows + piece * plan.relay_rows
    slot = rank - plan.slots + jnp.where(home, 0, plan.over)
    slots = 2 * plan.over
    base = jnp.where(
        direct, block_part * plan.direct_rows + rank * plan.full, origin + slot * plan.full
    )
    tail = jnp.where(
        direct,
        block_part * plan.direct_rows + plan.slots * plan.full + rank,
        origin + slots * plan.full + slot,
    )
    return base, tail, jnp.where(direct, plan.slots, slots)


def exchange(plan, room, table, adv, places, tile_perm):
    over = range(plan.devices)
    cross = pack_cross(plan, table, adv, room)
    crossed = lax.ppermute(cross, both, [(i, plan.partner(i)) for i in over])
    direct = pack_direct(plan, table, adv)
    arrived = lax.all_to_all(direct, both, split_axis=0, concat_axis=0, tiled=True)
    pieces = list(relay(plan, table, adv, crossed, room))
    for d in range(1, plan.mates):
        pairs = [(i, plan.device(plan.mate(i) ^ d, plan.half(i))) for i in over]
        pieces[d] = lax.ppermute(pieces[d], both, pairs)
    flat = arrived.reshape(plan.devices * plan.direct_rows, plan.width)
    return unpack(plan, places, tile_perm, flat, pieces)


def on_device(
    states, block_part, tile_perm, half_volt, steepness, gate_rate, conductance, reversal
):
    blocks, width = tile_perm.shape
    plan = Plan(states.shape[0], blocks, width)
    devices = plan.devices
    me = plan.me()
    ids = jnp.arange(devices, dtype=jnp.int32)
    onehot = (block_part[:, None] == ids[None, :]).astype(jnp.int32)
    counts = jnp.sum(onehot, axis=0, dtype=jnp.int32)
    told = jnp.broadcast_to(counts[None, :], (devices, devices))
    table = lax.all_to_all(told, both, split_axis=0, concat_axis=0, tiled=True)
    adv = advance(states, half_volt, steepness, gate_rate, conductance, reversal)
    far = plan.half(ids)[:, None] != plan.half(ids)[None, :]
    spilled = jnp.sum(jnp.where(far, jnp.maximum(table - plan.slots, 0), 0), axis=0)
    spilled = jnp.max(spilled)
    places = find_places(plan, block_part, me)
    rooms = [plan.worst * 3 // 8, plan.worst // 2, plan.worst]
    rooms = [round_up(room, sublanes) for room in rooms]
    choice = sum((spilled > room).astype(jnp.int32) for room in rooms[:-1])
    return lax.switch(
        choice,
        [functools.partial(exchange, plan, room) for room in rooms],
        table.reshape(-1),
        adv,
        places,
        tile_perm,
    )


def solution(mesh):
    return jax.shard_map(
        on_device,
        mesh=mesh,
        in_specs=(
            P(None, both),
            P(both),
            P(both, None),
            P(),
            P(),
            P(),
            P(),
            P(),
        ),
        out_specs=P(None, both),
        check_vma=False,
    )
```

```python
import functools

import jax
import jax.numpy as jnp
from jax import lax
from jax.experimental import pallas as pl
from jax.experimental.pallas import tpu as pltpu
from jax.sharding import PartitionSpec as P


time_step = 0.25
sublanes = 8
both = ("group", "peer")
smem_full = pl.BlockSpec(memory_space=pltpu.SMEM)
vmem_full = pl.BlockSpec(memory_space=pltpu.VMEM)
any_full = pl.BlockSpec(memory_space=pl.ANY)


def round_up(value, step):
    return -(-value // step) * step


class Plan:
    def __init__(self, rows, blocks, width):
        self.rows, self.blocks, self.width = rows, blocks, width
        self.peers = lax.axis_size("peer")
        self.devices = lax.axis_size("group") * self.peers
        self.near = self.peers // 2
        self.mates = self.devices // 2
        most = 2 * blocks // self.devices
        self.slots = max(most // 2, 1)
        self.over = most - self.slots
        self.full = rows // sublanes * sublanes
        self.extra = rows - self.full
        self.direct_rows = round_up(rows * self.slots, sublanes)
        self.spill_rows = round_up(rows * self.over, sublanes)
        self.worst = self.mates * self.over

    def half(self, device):
        return (device % self.peers) // self.near

    def mate(self, device):
        return device // self.peers * self.near + device % self.near

    def device(self, mate, half):
        return mate // self.near * self.peers + half * self.near + mate % self.near

    def partner(self, device):
        flip = 1 - 2 * self.half(device)
        return device + flip * self.near

    def me(self):
        return lax.axis_index("group") * self.peers + lax.axis_index("peer")


def advanced(params_ref, vals, tail):
    full = vals.shape[0]
    voltage = vals[0:1]
    relax = 1.5 + 0.5 * jnp.tanh(0.5 * voltage)
    done, current = [], 0.0
    for part, rows in ((vals, slice(0, full)), (tail, slice(full, None))):
        if part is None:
            continue
        steady = 0.5 + 0.5 * jnp.tanh((voltage - params_ref[0, rows]) * params_ref[1, rows])
        damping = jnp.exp(params_ref[2, rows] * relax)
        gates = steady + (part - steady) * damping
        drive = params_ref[3, rows] * gates * (voltage - params_ref[4, rows])
        current = current + jnp.sum(drive, axis=0, keepdims=True)
        done.append(gates)
    row = lax.broadcasted_iota(jnp.int32, vals.shape, 0)
    done[0] = jnp.where(row == 0, voltage - time_step * current, done[0])
    return done


def advance_kernel(params_ref, states_ref, out_ref, *, width):
    rows = states_ref.shape[0]
    full = rows // sublanes * sublanes

    def one(i, carry):
        cols = pl.ds(pl.multiple_of(i * width, width), width)
        tail = states_ref[full:rows, cols] if rows > full else None
        done = advanced(params_ref, states_ref[0:full, cols], tail)
        out_ref[0:full, cols] = done[0]
        if rows > full:
            out_ref[full:rows, cols] = done[1]
        return carry

    lax.fori_loop(0, states_ref.shape[1] // width, one, 0)


def gate_params(half_volt, steepness, gate_rate, conductance, reversal, width):
    params = jnp.stack([half_volt, 0.5 * steepness, -gate_rate, conductance, reversal])
    params = jnp.pad(params, ((0, 0), (1, 0)))
    return jnp.broadcast_to(params[:, :, None], params.shape + (width,))


def advance(params, states):
    rows, nodes = states.shape
    width = params.shape[2]
    block = fitting(nodes, 4096)
    return pl.pallas_call(
        functools.partial(advance_kernel, width=width),
        grid=(nodes // block,),
        in_specs=[
            pl.BlockSpec(params.shape, lambda i: (0, 0, 0)),
            pl.BlockSpec((rows, block), lambda i: (0, i)),
        ],
        out_specs=pl.BlockSpec((rows, block), lambda i: (0, i)),
        out_shape=jax.ShapeDtypeStruct(states.shape, states.dtype),
        cost_estimate=pl.CostEstimate(
            flops=40 * rows * nodes,
            bytes_accessed=8 * rows * nodes,
            transcendentals=3 * rows * nodes,
        ),
        name="advance",
    )(params, states)


def fitting(total, most):
    size = min(total, most)
    while total % size:
        size -= 128
    return size


def put_block(plan, adv_ref, block, put, base, tail):
    cols = pl.ds(pl.multiple_of(block * plan.width, plan.width), plan.width)
    put(base, plan.full, adv_ref[0 : plan.full, cols])
    for e in range(plan.extra):
        put(tail(e), 1, adv_ref[plan.full + e : plan.full + e + 1, cols])


def cross_kernel(table_ref, adv_ref, cross_ref, *, plan, room):
    me = plan.me()
    mine = plan.half(me)

    def one(s, carry):
        start, at = carry
        count = table_ref[s, 0, me]
        far = (plan.half(s) != mine).astype(jnp.int32)
        more = jnp.maximum(count - plan.slots, 0) * far

        def spill(k, carry):
            slot = jnp.minimum(at + k, room - 1)

            def put(base, size, vals):
                if size == plan.full:
                    base = pl.multiple_of(base, sublanes)
                cross_ref[pl.ds(base, size), :] = vals

            put_block(
                plan,
                adv_ref,
                start + plan.slots + k,
                put,
                slot * plan.full,
                lambda e: room * plan.full + e * room + slot,
            )
            return carry

        lax.fori_loop(0, more, spill, 0)
        return start + count, at + more

    lax.fori_loop(0, plan.devices, one, (0, 0))


def pack_cross(plan, table, adv, room):
    rows = round_up(room * plan.rows, sublanes)
    return pl.pallas_call(
        functools.partial(cross_kernel, plan=plan, room=room),
        in_specs=[smem_full, vmem_full],
        out_specs=vmem_full,
        out_shape=jax.ShapeDtypeStruct((rows, plan.width), adv.dtype),
        name="pack_cross",
    )(table, adv)


def starts(plan, table_ref, start_ref):
    me = plan.me()

    def scan(s, start):
        start_ref[s] = start
        return start + table_ref[s, 0, me]

    lax.fori_loop(0, plan.devices, scan, 0)


def slots_kernel(table_ref, adv_ref, out_ref, start_ref, *, plan, inner):
    per_step = out_ref.shape[0]
    first = pl.program_id(0) * per_step
    slots = plan.over if inner else plan.slots

    @pl.when(first == 0)
    def _():
        starts(plan, table_ref, start_ref)

    for d in range(per_step):
        to = first + d
        if inner:
            start = start_ref[plan.device(to, plan.half(plan.me()))] + plan.slots
        else:
            start = start_ref[to]

        def put(base, size, vals):
            out_ref[d, base : base + size, :] = vals

        for k in range(slots):
            put_block(
                plan,
                adv_ref,
                jnp.minimum(start + k, plan.blocks - 1),
                put,
                k * plan.full,
                lambda e: slots * plan.full + e * slots + k,
            )


def pack_slots(plan, table, adv, inner):
    count = plan.mates if inner else plan.devices
    rows = plan.spill_rows if inner else plan.direct_rows
    per_step = fitting_blocks(count, 4)
    return pl.pallas_call(
        functools.partial(slots_kernel, plan=plan, inner=inner),
        grid_spec=pltpu.PrefetchScalarGridSpec(
            num_scalar_prefetch=1,
            grid=(count // per_step,),
            in_specs=[pl.BlockSpec(adv.shape, lambda i, *_: (0, 0))],
            out_specs=pl.BlockSpec((per_step, rows, plan.width), lambda i, *_: (i, 0, 0)),
            scratch_shapes=[pltpu.SMEM((plan.devices,), jnp.int32)],
        ),
        out_shape=jax.ShapeDtypeStruct((count, rows, plan.width), adv.dtype),
        name="pack_inner" if inner else "pack_direct",
    )(table, adv)


def relay_kernel(table_ref, params_ref, cross_ref, *refs, plan, room):
    outs, (far_ref, done_ref) = refs[: plan.mates], refs[plan.mates :]
    me = plan.me()
    mine = plan.half(me)
    other = plan.partner(me)

    def scan(s, at):
        far_ref[s] = at
        near = (plan.half(s) == mine).astype(jnp.int32)
        return at + jnp.maximum(table_ref[s, 0, other] - plan.slots, 0) * near

    total = lax.fori_loop(0, plan.devices, scan, 0)

    def step(i, carry):
        rows = pl.ds(pl.multiple_of(i * plan.full, plan.full), plan.full)
        tails = [pl.ds(room * plan.full + e * room + i, 1) for e in range(plan.extra)]
        tail = None
        if tails:
            tail = jnp.concatenate([cross_ref[t, :] for t in tails], axis=0)
        done = advanced(params_ref, cross_ref[rows, :], tail)
        done_ref[rows, :] = done[0]
        for e, t in enumerate(tails):
            done_ref[t, :] = done[1][e : e + 1]
        return carry

    lax.fori_loop(0, jnp.minimum(total, room), step, 0)
    here = plan.mate(me)
    slots = plan.over
    for d, out_ref in enumerate(outs):
        at = far_ref[plan.device(here ^ d, mine)]
        for k in range(slots):
            slot = jnp.minimum(at + k, room - 1)
            out_ref[k * plan.full : (k + 1) * plan.full, :] = done_ref[
                pl.ds(pl.multiple_of(slot * plan.full, plan.full), plan.full), :
            ]
            for e in range(plan.extra):
                row = slots * plan.full + e * slots + k
                out_ref[row : row + 1, :] = done_ref[
                    pl.ds(room * plan.full + e * room + slot, 1), :
                ]


def relay(plan, table, params, crossed, room):
    piece = jax.ShapeDtypeStruct((plan.spill_rows, plan.width), crossed.dtype)
    return pl.pallas_call(
        functools.partial(relay_kernel, plan=plan, room=room),
        in_specs=[smem_full, vmem_full, vmem_full],
        out_specs=[vmem_full] * plan.mates,
        out_shape=[piece] * plan.mates,
        scratch_shapes=[
            pltpu.SMEM((plan.devices,), jnp.int32),
            pltpu.VMEM(crossed.shape, crossed.dtype),
        ],
        name="relay",
    )(table, params, crossed)


def permuted(vals, lanes):
    return jnp.take_along_axis(vals, lanes, axis=1, mode="promise_in_bounds")


def unpack_kernel(
    base_ref, tail_ref, step_ref, perm_ref, direct_ref, inner_ref, *refs, plan
):
    pieces = refs[: plan.mates]
    out_ref, got_ref, last_ref, sem = refs[plan.mates :]
    per_step, width = perm_ref.shape
    first = pl.program_id(0) * per_step

    @pl.when(first == 0)
    def _():
        direct = plan.devices * plan.direct_rows
        inner = plan.mates * plan.spill_rows
        sizes = [direct, inner] + [plan.spill_rows] * plan.mates
        copies, at = [], 0
        for i, (src_ref, size) in enumerate(zip([direct_ref, inner_ref, *pieces], sizes)):
            rows = pl.ds(at, size)
            copies.append(pltpu.make_async_copy(src_ref, got_ref.at[rows], sem.at[i]))
            at += size
        for copy in copies:
            copy.start()
        for copy in copies:
            copy.wait()

    for i in range(per_step):
        base = pl.multiple_of(base_ref[first + i], sublanes)
        tail = tail_ref[first + i]
        stride = step_ref[first + i]
        lanes = jnp.broadcast_to(perm_ref[i : i + 1, :], (plan.full, width))
        vals = got_ref[pl.ds(base, plan.full), :]
        out_ref[0 : plan.full, i * width : (i + 1) * width] = permuted(vals, lanes)
        for e in range(plan.extra):
            last_ref[e, i : i + 1, :] = got_ref[pl.ds(tail + e * stride, 1), :]
    for e in range(plan.extra):
        last = permuted(last_ref[e], perm_ref[...])
        for i in range(per_step):
            cols = slice(i * width, (i + 1) * width)
            out_ref[plan.full + e : plan.full + e + 1, cols] = last[i : i + 1, :]


def unpack(plan, places, perm, direct, inner, pieces):
    per_step = fitting_blocks(plan.blocks, 16)
    total = plan.devices * plan.direct_rows + 2 * plan.mates * plan.spill_rows
    return pl.pallas_call(
        functools.partial(unpack_kernel, plan=plan),
        grid_spec=pltpu.PrefetchScalarGridSpec(
            num_scalar_prefetch=3,
            grid=(plan.blocks // per_step,),
            in_specs=[pl.BlockSpec((per_step, plan.width), lambda i, *_: (i, 0))]
            + [any_full] * (2 + plan.mates),
            out_specs=pl.BlockSpec((plan.rows, per_step * plan.width), lambda i, *_: (0, i)),
            scratch_shapes=[
                pltpu.VMEM((total, plan.width), direct.dtype),
                pltpu.VMEM((max(plan.extra, 1), per_step, plan.width), direct.dtype),
                pltpu.SemaphoreType.DMA((2 + plan.mates,)),
            ],
        ),
        out_shape=jax.ShapeDtypeStruct((plan.rows, plan.blocks * plan.width), direct.dtype),
        name="unpack",
    )(*places, perm, direct, inner, *pieces)


def fitting_blocks(total, most):
    size = min(total, most)
    while total % size:
        size -= 1
    return size


def find_places(plan, block_part, me):
    same = block_part[:, None] == block_part[None, :]
    position = jnp.arange(plan.blocks, dtype=jnp.int32)
    ahead = position[None, :] < position[:, None]
    rank = jnp.sum((same & ahead).astype(jnp.int32), axis=1, dtype=jnp.int32)
    direct = rank < plan.slots
    home = plan.half(block_part) == plan.half(me)
    mate = plan.mate(block_part)
    piece = jnp.where(home, mate, plan.mates + (mate ^ plan.mate(me)))
    origin = plan.devices * plan.direct_rows + piece * plan.spill_rows
    slot = rank - plan.slots
    base = jnp.where(
        direct, block_part * plan.direct_rows + rank * plan.full, origin + slot * plan.full
    )
    tail = jnp.where(
        direct,
        block_part * plan.direct_rows + plan.slots * plan.full + rank,
        origin + plan.over * plan.full + slot,
    )
    return base, tail, jnp.where(direct, plan.slots, plan.over)


def exchange(plan, room, table, states, params, places, tile_perm):
    over = range(plan.devices)
    halves = [[plan.device(m, h) for m in range(plan.mates)] for h in range(2)]
    cross = pack_cross(plan, table, states, room)
    crossed = lax.ppermute(cross, both, [(i, plan.partner(i)) for i in over])
    adv = advance(params, states)
    inner = pack_slots(plan, table, adv, True)
    inner = lax.all_to_all(
        inner, both, split_axis=0, concat_axis=0, tiled=True, axis_index_groups=halves
    )
    direct = pack_slots(plan, table, adv, False)
    direct, crossed = lax.optimization_barrier((direct, crossed))
    direct = lax.all_to_all(direct, both, split_axis=0, concat_axis=0, tiled=True)
    pieces = list(relay(plan, table, params, crossed, room))
    for d in range(1, plan.mates):
        pairs = [(i, plan.device(plan.mate(i) ^ d, plan.half(i))) for i in over]
        pieces[d] = lax.ppermute(pieces[d], both, pairs)
    direct = direct.reshape(plan.devices * plan.direct_rows, plan.width)
    inner = inner.reshape(plan.mates * plan.spill_rows, plan.width)
    return unpack(plan, places, tile_perm, direct, inner, pieces)


def on_device(
    states, block_part, tile_perm, half_volt, steepness, gate_rate, conductance, reversal
):
    blocks, width = tile_perm.shape
    plan = Plan(states.shape[0], blocks, width)
    devices = plan.devices
    me = plan.me()
    ids = jnp.arange(devices, dtype=jnp.int32)
    onehot = (block_part[:, None] == ids[None, :]).astype(jnp.int32)
    counts = jnp.sum(onehot, axis=0, dtype=jnp.int32)
    told = jnp.broadcast_to(counts[None, None, :], (devices, 1, devices))
    table = lax.all_to_all(told, both, split_axis=0, concat_axis=0, tiled=True)
    params = gate_params(half_volt, steepness, gate_rate, conductance, reversal, width)
    far = plan.half(ids)[:, None] != plan.half(ids)[None, :]
    spilled = jnp.maximum(table - plan.slots, 0)
    spilled = jnp.sum(jnp.where(far[:, None, :], spilled, 0), axis=0)
    spilled = jnp.max(spilled)
    places = find_places(plan, block_part, me)
    rooms = [plan.worst * 3 // 8, plan.worst // 2, plan.worst]
    rooms = [round_up(room, sublanes) for room in rooms]
    choice = sum((spilled > room).astype(jnp.int32) for room in rooms[:-1])
    return lax.switch(
        choice,
        [functools.partial(exchange, plan, room) for room in rooms],
        table,
        states,
        params,
        places,
        tile_perm,
    )


def solution(mesh):
    return jax.shard_map(
        on_device,
        mesh=mesh,
        in_specs=(
            P(None, both),
            P(both),
            P(both, None),
            P(),
            P(),
            P(),
            P(),
            P(),
        ),
        out_specs=P(None, both),
        check_vma=False,
    )
```

```python
import functools

import jax
import jax.numpy as jnp
from jax import lax
from jax.experimental import pallas as pl
from jax.experimental.pallas import tpu as pltpu
from jax.sharding import PartitionSpec as P


time_step = 0.25
sublanes = 8
both = ("group", "peer")
smem_full = pl.BlockSpec(memory_space=pltpu.SMEM)
vmem_full = pl.BlockSpec(memory_space=pltpu.VMEM)
any_full = pl.BlockSpec(memory_space=pl.ANY)


def round_up(value, step):
    return -(-value // step) * step


class Plan:
    def __init__(self, rows, blocks, width):
        self.rows, self.blocks, self.width = rows, blocks, width
        self.peers = lax.axis_size("peer")
        self.devices = lax.axis_size("group") * self.peers
        self.near = self.peers // 2
        self.mates = self.devices // 2
        most = 2 * blocks // self.devices
        self.slots = max(most // 2, 1)
        self.over = most - self.slots
        self.full = rows // sublanes * sublanes
        self.extra = rows - self.full
        self.most = self.slots + self.over
        self.inner_rows = round_up(rows * self.most, sublanes)
        self.cross_rows = round_up(rows * self.slots, sublanes)
        self.relay_rows = round_up(rows * self.over, sublanes)
        self.chunk = 16
        self.chunk_rows = round_up(rows * self.chunk, sublanes)
        self.worst = self.mates * self.over

    def half(self, device):
        return (device % self.peers) // self.near

    def mate(self, device):
        return device // self.peers * self.near + device % self.near

    def device(self, mate, half):
        return mate // self.near * self.peers + half * self.near + mate % self.near

    def partner(self, device):
        flip = 1 - 2 * self.half(device)
        return device + flip * self.near

    def me(self):
        return lax.axis_index("group") * self.peers + lax.axis_index("peer")


def advanced(params_ref, vals, tail):
    full = vals.shape[0]
    voltage = vals[0:1]
    relax = 1.5 + 0.5 * jnp.tanh(0.5 * voltage)
    done, current = [], 0.0
    for part, rows in ((vals, slice(0, full)), (tail, slice(full, None))):
        if part is None:
            continue
        steady = 0.5 + 0.5 * jnp.tanh((voltage - params_ref[0, rows]) * params_ref[1, rows])
        damping = jnp.exp(params_ref[2, rows] * relax)
        gates = steady + (part - steady) * damping
        drive = params_ref[3, rows] * gates * (voltage - params_ref[4, rows])
        current = current + jnp.sum(drive, axis=0, keepdims=True)
        done.append(gates)
    row = lax.broadcasted_iota(jnp.int32, vals.shape, 0)
    done[0] = jnp.where(row == 0, voltage - time_step * current, done[0])
    return done


def advance_kernel(params_ref, states_ref, out_ref, *, width):
    rows = states_ref.shape[0]
    full = rows // sublanes * sublanes

    def one(i, carry):
        cols = pl.ds(pl.multiple_of(i * width, width), width)
        tail = states_ref[full:rows, cols] if rows > full else None
        done = advanced(params_ref, states_ref[0:full, cols], tail)
        out_ref[0:full, cols] = done[0]
        if rows > full:
            out_ref[full:rows, cols] = done[1]
        return carry

    lax.fori_loop(0, states_ref.shape[1] // width, one, 0)


def gate_params(half_volt, steepness, gate_rate, conductance, reversal, width):
    params = jnp.stack([half_volt, 0.5 * steepness, -gate_rate, conductance, reversal])
    params = jnp.pad(params, ((0, 0), (1, 0)))
    return jnp.broadcast_to(params[:, :, None], params.shape + (width,))


def advance(params, states):
    rows, nodes = states.shape
    width = params.shape[2]
    block = fitting(nodes, 4096)
    return pl.pallas_call(
        functools.partial(advance_kernel, width=width),
        grid=(nodes // block,),
        in_specs=[
            pl.BlockSpec(params.shape, lambda i: (0, 0, 0)),
            pl.BlockSpec((rows, block), lambda i: (0, i)),
        ],
        out_specs=pl.BlockSpec((rows, block), lambda i: (0, i)),
        out_shape=jax.ShapeDtypeStruct(states.shape, states.dtype),
        cost_estimate=pl.CostEstimate(
            flops=40 * rows * nodes,
            bytes_accessed=8 * rows * nodes,
            transcendentals=3 * rows * nodes,
        ),
        name="advance",
    )(params, states)


def fitting(total, most):
    size = min(total, most)
    while total % size:
        size -= 128
    return size


def put_block(plan, adv_ref, block, put, base, tail):
    cols = pl.ds(pl.multiple_of(block * plan.width, plan.width), plan.width)
    put(base, plan.full, adv_ref[0 : plan.full, cols])
    for e in range(plan.extra):
        put(tail(e), 1, adv_ref[plan.full + e : plan.full + e + 1, cols])


def dense_kernel(table_ref, states_ref, *refs, plan):
    outs, all_ref = refs[:-1], refs[-1]
    room = len(outs) * plan.chunk
    me = plan.me()
    mine = plan.half(me)

    def one(s, carry):
        start, at = carry
        count = table_ref[s, 0, me]
        far = (plan.half(s) != mine).astype(jnp.int32)
        more = jnp.maximum(count - plan.slots, 0) * far

        def spill(k, carry):
            slot = jnp.minimum(at + k, room - 1)

            def put(base, size, vals):
                if size == plan.full:
                    base = pl.multiple_of(base, sublanes)
                all_ref[pl.ds(base, size), :] = vals

            put_block(
                plan,
                states_ref,
                start + plan.slots + k,
                put,
                slot * plan.full,
                lambda e: room * plan.full + e * room + slot,
            )
            return carry

        lax.fori_loop(0, more, spill, 0)
        return start + count, at + more

    lax.fori_loop(0, plan.devices, one, (0, 0))
    for c, out_ref in enumerate(outs):
        size = plan.chunk * plan.full
        out_ref[0:size, :] = all_ref[c * size : (c + 1) * size, :]
        for e in range(plan.extra):
            row = room * plan.full + e * room + c * plan.chunk
            to = size + e * plan.chunk
            out_ref[to : to + plan.chunk, :] = all_ref[row : row + plan.chunk, :]


def pack_dense(plan, table, states, chunks):
    piece = jax.ShapeDtypeStruct((plan.chunk_rows, plan.width), states.dtype)
    rows = round_up(chunks * plan.chunk * plan.rows, sublanes)
    return pl.pallas_call(
        functools.partial(dense_kernel, plan=plan),
        in_specs=[smem_full, vmem_full],
        out_specs=[vmem_full] * chunks,
        out_shape=[piece] * chunks,
        scratch_shapes=[pltpu.VMEM((rows, plan.width), states.dtype)],
        name="pack_dense",
    )(table, states)


def pieces_kernel(table_ref, adv_ref, *refs, plan, inner, cross):
    outs, start_ref = refs[:-1], refs[-1]
    me = plan.me()
    mine = plan.half(me)
    here = plan.mate(me)

    def scan(s, start):
        start_ref[s] = start
        return start + table_ref[s, 0, me]

    lax.fori_loop(0, plan.devices, scan, 0)
    jobs = [(d, mine, plan.most) for d in inner] + [(d, 1 - mine, plan.slots) for d in cross]
    for (d, half, slots), out_ref in zip(jobs, outs):
        start = start_ref[plan.device(here ^ d, half)]

        def put(base, size, vals):
            out_ref[base : base + size, :] = vals

        for k in range(slots):
            put_block(
                plan,
                adv_ref,
                jnp.minimum(start + k, plan.blocks - 1),
                put,
                k * plan.full,
                lambda e: slots * plan.full + e * slots + k,
            )


def pack_pieces(plan, table, adv, inner, cross):
    rows = [plan.inner_rows] * len(inner) + [plan.cross_rows] * len(cross)
    return pl.pallas_call(
        functools.partial(pieces_kernel, plan=plan, inner=inner, cross=cross),
        in_specs=[smem_full, vmem_full],
        out_specs=[vmem_full] * len(rows),
        out_shape=[jax.ShapeDtypeStruct((size, plan.width), adv.dtype) for size in rows],
        scratch_shapes=[pltpu.SMEM((plan.devices,), jnp.int32)],
    )(table, adv)


def relay_kernel(table_ref, params_ref, *refs, plan, chunks):
    dense, outs = refs[:chunks], refs[chunks : chunks + plan.mates]
    far_ref, done_ref = refs[chunks + plan.mates :]
    room = chunks * plan.chunk
    me = plan.me()
    mine = plan.half(me)
    other = plan.partner(me)

    def scan(s, at):
        far_ref[s] = at
        near = (plan.half(s) == mine).astype(jnp.int32)
        return at + jnp.maximum(table_ref[s, 0, other] - plan.slots, 0) * near

    total = lax.fori_loop(0, plan.devices, scan, 0)
    for c, dense_ref in enumerate(dense):

        def step(i, carry):
            rows = pl.ds(pl.multiple_of(i * plan.full, plan.full), plan.full)
            tail = None
            if plan.extra:
                lasts = [plan.chunk * plan.full + e * plan.chunk + i for e in range(plan.extra)]
                tail = [dense_ref[pl.ds(last, 1), :] for last in lasts]
                tail = jnp.concatenate(tail, axis=0) if plan.extra > 1 else tail[0]
            done = advanced(params_ref, dense_ref[rows, :], tail)
            slot = c * plan.chunk + i
            to = pl.ds(pl.multiple_of(slot * plan.full, plan.full), plan.full)
            done_ref[to, :] = done[0]
            for e in range(plan.extra):
                row = room * plan.full + e * room + slot
                done_ref[pl.ds(row, 1), :] = done[1][e : e + 1]
            return carry

        lax.fori_loop(0, jnp.clip(total - c * plan.chunk, 0, plan.chunk), step, 0)
    here = plan.mate(me)
    slots = plan.over
    for d, out_ref in enumerate(outs):
        at = far_ref[plan.device(here ^ d, mine)]
        for k in range(slots):
            slot = jnp.minimum(at + k, room - 1)
            out_ref[k * plan.full : (k + 1) * plan.full, :] = done_ref[
                pl.ds(pl.multiple_of(slot * plan.full, plan.full), plan.full), :
            ]
            for e in range(plan.extra):
                row = slots * plan.full + e * slots + k
                out_ref[row : row + 1, :] = done_ref[
                    pl.ds(room * plan.full + e * room + slot, 1), :
                ]


def relay(plan, table, params, dense):
    piece = jax.ShapeDtypeStruct((plan.relay_rows, plan.width), dense[0].dtype)
    rows = round_up(len(dense) * plan.chunk * plan.rows, sublanes)
    return pl.pallas_call(
        functools.partial(relay_kernel, plan=plan, chunks=len(dense)),
        in_specs=[smem_full] + [vmem_full] * (1 + len(dense)),
        out_specs=[vmem_full] * plan.mates,
        out_shape=[piece] * plan.mates,
        scratch_shapes=[
            pltpu.SMEM((plan.devices,), jnp.int32),
            pltpu.VMEM((rows, plan.width), dense[0].dtype),
        ],
        name="relay",
    )(table, params, *dense)


def permuted(vals, lanes):
    return jnp.take_along_axis(vals, lanes, axis=1, mode="promise_in_bounds")


def unpack_kernel(base_ref, tail_ref, step_ref, perm_ref, *refs, plan, sizes):
    pieces = refs[: len(sizes)]
    out_ref, got_ref, last_ref, sem = refs[len(sizes) :]
    per_step, width = perm_ref.shape
    first = pl.program_id(0) * per_step

    @pl.when(first == 0)
    def _():
        copies, at = [], 0
        for i, (piece_ref, size) in enumerate(zip(pieces, sizes)):
            rows = pl.ds(at, size)
            copies.append(pltpu.make_async_copy(piece_ref, got_ref.at[rows], sem.at[i]))
            at += size
        for copy in copies:
            copy.start()
        for copy in copies:
            copy.wait()

    for i in range(per_step):
        base = pl.multiple_of(base_ref[first + i], sublanes)
        tail = tail_ref[first + i]
        stride = step_ref[first + i]
        lanes = jnp.broadcast_to(perm_ref[i : i + 1, :], (plan.full, width))
        vals = got_ref[pl.ds(base, plan.full), :]
        out_ref[0 : plan.full, i * width : (i + 1) * width] = permuted(vals, lanes)
        for e in range(plan.extra):
            last_ref[e, i : i + 1, :] = got_ref[pl.ds(tail + e * stride, 1), :]
    for e in range(plan.extra):
        last = permuted(last_ref[e], perm_ref[...])
        for i in range(per_step):
            cols = slice(i * width, (i + 1) * width)
            out_ref[plan.full + e : plan.full + e + 1, cols] = last[i : i + 1, :]


def unpack(plan, places, perm, pieces):
    per_step = fitting_blocks(plan.blocks, 16)
    sizes = [piece.shape[0] for piece in pieces]
    dtype = pieces[0].dtype
    return pl.pallas_call(
        functools.partial(unpack_kernel, plan=plan, sizes=sizes),
        grid_spec=pltpu.PrefetchScalarGridSpec(
            num_scalar_prefetch=3,
            grid=(plan.blocks // per_step,),
            in_specs=[pl.BlockSpec((per_step, plan.width), lambda i, *_: (i, 0))]
            + [any_full] * len(pieces),
            out_specs=pl.BlockSpec((plan.rows, per_step * plan.width), lambda i, *_: (0, i)),
            scratch_shapes=[
                pltpu.VMEM((sum(sizes), plan.width), dtype),
                pltpu.VMEM((max(plan.extra, 1), per_step, plan.width), dtype),
                pltpu.SemaphoreType.DMA((len(pieces),)),
            ],
        ),
        out_shape=jax.ShapeDtypeStruct((plan.rows, plan.blocks * plan.width), dtype),
        name="unpack",
    )(*places, perm, *pieces)


def fitting_blocks(total, most):
    size = min(total, most)
    while total % size:
        size -= 1
    return size


def find_places(plan, block_part, me):
    same = block_part[:, None] == block_part[None, :]
    position = jnp.arange(plan.blocks, dtype=jnp.int32)
    ahead = position[None, :] < position[:, None]
    rank = jnp.sum((same & ahead).astype(jnp.int32), axis=1, dtype=jnp.int32)
    home = plan.half(block_part) == plan.half(me)
    direct = rank < plan.slots
    piece = plan.mate(block_part) ^ plan.mate(me)
    crossed = plan.mates * plan.inner_rows + piece * plan.cross_rows
    relayed = plan.mates * (plan.inner_rows + plan.cross_rows) + piece * plan.relay_rows
    origin = jnp.where(home, piece * plan.inner_rows, jnp.where(direct, crossed, relayed))
    slots = jnp.where(home, plan.most, jnp.where(direct, plan.slots, plan.over))
    slot = jnp.where(home | direct, rank, rank - plan.slots)
    return origin + slot * plan.full, origin + slots * plan.full + slot, slots


def exchange(plan, chunks, table, states, params, places, tile_perm):
    over = range(plan.devices)
    split = plan.mates // 2
    ends = {"inner": plan.half, "again": plan.half, "cross": lambda i: 1 - plan.half(i)}

    def send(kind, d, piece):
        pairs = [(i, plan.device(plan.mate(i) ^ d, ends[kind](i))) for i in over]
        return lax.ppermute(piece, both, pairs)

    dense = pack_dense(plan, table, states, chunks)
    crossed = []
    for c in range(chunks):
        crossed.append(
            lax.ppermute(dense[c], both, [(i, plan.partner(i)) for i in over])
        )
    adv = advance(params, states)
    first = list(range(1, split))
    second = [0] + list(range(split, plan.mates))
    inner = dict(zip(first, pack_pieces(plan, table, adv, first, [])))
    more = pack_pieces(plan, table, adv, second, list(range(plan.mates)))
    inner.update(zip(second, more))
    cross = list(more[len(second) :])
    again = list(relay(plan, table, params, crossed))
    for d in range(plan.mates):
        cross[d] = send("cross", d, cross[d])
        if d:
            inner[d] = send("inner", d, inner[d])
            again[d] = send("again", d, again[d])
    inner = [inner[d] for d in range(plan.mates)]
    return unpack(plan, places, tile_perm, [*inner, *cross, *again])


def on_device(
    states, block_part, tile_perm, half_volt, steepness, gate_rate, conductance, reversal
):
    blocks, width = tile_perm.shape
    plan = Plan(states.shape[0], blocks, width)
    devices = plan.devices
    me = plan.me()
    ids = jnp.arange(devices, dtype=jnp.int32)
    onehot = (block_part[:, None] == ids[None, :]).astype(jnp.int32)
    counts = jnp.sum(onehot, axis=0, dtype=jnp.int32)
    told = jnp.broadcast_to(counts[None, None, :], (devices, 1, devices))
    table = lax.all_to_all(told, both, split_axis=0, concat_axis=0, tiled=True)
    params = gate_params(half_volt, steepness, gate_rate, conductance, reversal, width)
    far = plan.half(ids)[:, None] != plan.half(ids)[None, :]
    spilled = jnp.maximum(table - plan.slots, 0)
    spilled = jnp.sum(jnp.where(far[:, None, :], spilled, 0), axis=0)
    spilled = jnp.max(spilled)
    places = find_places(plan, block_part, me)
    most = -(-plan.worst // plan.chunk)
    rooms = sorted({-(-most * 3 // 8), -(-most // 2), most})
    choice = sum((spilled > room * plan.chunk).astype(jnp.int32) for room in rooms[:-1])
    choice = jnp.asarray(choice, jnp.int32)
    return lax.switch(
        choice,
        [functools.partial(exchange, plan, room) for room in rooms],
        table,
        states,
        params,
        places,
        tile_perm,
    )


def solution(mesh):
    return jax.shard_map(
        on_device,
        mesh=mesh,
        in_specs=(
            P(None, both),
            P(both),
            P(both, None),
            P(),
            P(),
            P(),
            P(),
            P(),
        ),
        out_specs=P(None, both),
        check_vma=False,
    )
```

```python
import functools

import jax
import jax.numpy as jnp
from jax import lax
from jax.experimental import pallas as pl
from jax.experimental.pallas import tpu as pltpu
from jax.sharding import PartitionSpec as P


time_step = 0.25
sublanes = 8
both = ("group", "peer")
smem_full = pl.BlockSpec(memory_space=pltpu.SMEM)
vmem_full = pl.BlockSpec(memory_space=pltpu.VMEM)
any_full = pl.BlockSpec(memory_space=pl.ANY)


def round_up(value, step):
    return -(-value // step) * step


class Plan:
    def __init__(self, rows, blocks, width):
        self.rows, self.blocks, self.width = rows, blocks, width
        self.peers = lax.axis_size("peer")
        self.devices = lax.axis_size("group") * self.peers
        self.near = self.peers // 2
        self.mates = self.devices // 2
        most = 2 * blocks // self.devices
        self.slots = max(most // 2, 1)
        self.over = most - self.slots
        self.full = rows // sublanes * sublanes
        self.extra = rows - self.full
        self.most = self.slots + self.over
        self.inner_rows = round_up(rows * self.most, sublanes)
        self.cross_rows = round_up(rows * self.slots, sublanes)
        self.relay_rows = round_up(rows * self.over, sublanes)
        self.chunk = 16
        self.chunk_rows = round_up(rows * self.chunk, sublanes)
        self.worst = self.mates * self.over

    def half(self, device):
        return (device % self.peers) // self.near

    def mate(self, device):
        return device // self.peers * self.near + device % self.near

    def device(self, mate, half):
        return mate // self.near * self.peers + half * self.near + mate % self.near

    def partner(self, device):
        flip = 1 - 2 * self.half(device)
        return device + flip * self.near

    def me(self):
        return lax.axis_index("group") * self.peers + lax.axis_index("peer")


def advanced(params_ref, vals, tail):
    full = vals.shape[0]
    voltage = vals[0:1]
    relax = 1.5 + 0.5 * jnp.tanh(0.5 * voltage)
    done, current = [], 0.0
    for part, rows in ((vals, slice(0, full)), (tail, slice(full, None))):
        if part is None:
            continue
        steady = 0.5 + 0.5 * jnp.tanh((voltage - params_ref[0, rows]) * params_ref[1, rows])
        damping = jnp.exp(params_ref[2, rows] * relax)
        gates = steady + (part - steady) * damping
        drive = params_ref[3, rows] * gates * (voltage - params_ref[4, rows])
        current = current + jnp.sum(drive, axis=0, keepdims=True)
        done.append(gates)
    row = lax.broadcasted_iota(jnp.int32, vals.shape, 0)
    done[0] = jnp.where(row == 0, voltage - time_step * current, done[0])
    return done


def advance_kernel(params_ref, states_ref, out_ref, *, width):
    rows = states_ref.shape[0]
    full = rows // sublanes * sublanes

    def one(i, carry):
        cols = pl.ds(pl.multiple_of(i * width, width), width)
        tail = states_ref[full:rows, cols] if rows > full else None
        done = advanced(params_ref, states_ref[0:full, cols], tail)
        out_ref[0:full, cols] = done[0]
        if rows > full:
            out_ref[full:rows, cols] = done[1]
        return carry

    lax.fori_loop(0, states_ref.shape[1] // width, one, 0)


def gate_params(half_volt, steepness, gate_rate, conductance, reversal, width):
    params = jnp.stack([half_volt, 0.5 * steepness, -gate_rate, conductance, reversal])
    params = jnp.pad(params, ((0, 0), (1, 0)))
    return jnp.broadcast_to(params[:, :, None], params.shape + (width,))


def advance(params, states):
    rows, nodes = states.shape
    width = params.shape[2]
    block = fitting(nodes, 4096)
    return pl.pallas_call(
        functools.partial(advance_kernel, width=width),
        grid=(nodes // block,),
        in_specs=[
            pl.BlockSpec(params.shape, lambda i: (0, 0, 0)),
            pl.BlockSpec((rows, block), lambda i: (0, i)),
        ],
        out_specs=pl.BlockSpec((rows, block), lambda i: (0, i)),
        out_shape=jax.ShapeDtypeStruct(states.shape, states.dtype),
        cost_estimate=pl.CostEstimate(
            flops=40 * rows * nodes,
            bytes_accessed=8 * rows * nodes,
            transcendentals=3 * rows * nodes,
        ),
        name="advance",
    )(params, states)


def fitting(total, most):
    size = min(total, most)
    while total % size:
        size -= 128
    return size


def put_block(plan, adv_ref, block, put, base, tail):
    cols = pl.ds(pl.multiple_of(block * plan.width, plan.width), plan.width)
    put(base, plan.full, adv_ref[0 : plan.full, cols])
    for e in range(plan.extra):
        put(tail(e), 1, adv_ref[plan.full + e : plan.full + e + 1, cols])


def dense_kernel(table_ref, states_ref, *refs, plan):
    outs, all_ref = refs[:-1], refs[-1]
    room = len(outs) * plan.chunk
    me = plan.me()
    mine = plan.half(me)

    def one(s, carry):
        start, at = carry
        count = table_ref[s, 0, me]
        far = (plan.half(s) != mine).astype(jnp.int32)
        more = jnp.maximum(count - plan.slots, 0) * far

        def spill(k, carry):
            slot = jnp.minimum(at + k, room - 1)

            def put(base, size, vals):
                if size == plan.full:
                    base = pl.multiple_of(base, sublanes)
                all_ref[pl.ds(base, size), :] = vals

            put_block(
                plan,
                states_ref,
                start + plan.slots + k,
                put,
                slot * plan.full,
                lambda e: room * plan.full + e * room + slot,
            )
            return carry

        lax.fori_loop(0, more, spill, 0)
        return start + count, at + more

    lax.fori_loop(0, plan.devices, one, (0, 0))
    for c, out_ref in enumerate(outs):
        size = plan.chunk * plan.full
        out_ref[0:size, :] = all_ref[c * size : (c + 1) * size, :]
        for e in range(plan.extra):
            row = room * plan.full + e * room + c * plan.chunk
            to = size + e * plan.chunk
            out_ref[to : to + plan.chunk, :] = all_ref[row : row + plan.chunk, :]


def pack_dense(plan, table, states, chunks):
    piece = jax.ShapeDtypeStruct((plan.chunk_rows, plan.width), states.dtype)
    rows = round_up(chunks * plan.chunk * plan.rows, sublanes)
    return pl.pallas_call(
        functools.partial(dense_kernel, plan=plan),
        in_specs=[smem_full, vmem_full],
        out_specs=[vmem_full] * chunks,
        out_shape=[piece] * chunks,
        scratch_shapes=[pltpu.VMEM((rows, plan.width), states.dtype)],
        name="pack_dense",
    )(table, states)


def pieces_kernel(table_ref, adv_ref, *refs, plan, inner, cross):
    outs, start_ref = refs[:-1], refs[-1]
    me = plan.me()
    mine = plan.half(me)
    here = plan.mate(me)

    def scan(s, start):
        start_ref[s] = start
        return start + table_ref[s, 0, me]

    lax.fori_loop(0, plan.devices, scan, 0)
    jobs = [(d, mine, plan.most) for d in inner] + [(d, 1 - mine, plan.slots) for d in cross]
    for (d, half, slots), out_ref in zip(jobs, outs):
        start = start_ref[plan.device(here ^ d, half)]

        def put(base, size, vals):
            out_ref[base : base + size, :] = vals

        for k in range(slots):
            put_block(
                plan,
                adv_ref,
                jnp.minimum(start + k, plan.blocks - 1),
                put,
                k * plan.full,
                lambda e: slots * plan.full + e * slots + k,
            )


def pack_pieces(plan, table, adv, inner, cross):
    rows = [plan.inner_rows] * len(inner) + [plan.cross_rows] * len(cross)
    return pl.pallas_call(
        functools.partial(pieces_kernel, plan=plan, inner=inner, cross=cross),
        in_specs=[smem_full, vmem_full],
        out_specs=[vmem_full] * len(rows),
        out_shape=[jax.ShapeDtypeStruct((size, plan.width), adv.dtype) for size in rows],
        scratch_shapes=[pltpu.SMEM((plan.devices,), jnp.int32)],
    )(table, adv)


def relay_kernel(table_ref, params_ref, *refs, plan, chunks):
    dense, outs = refs[:chunks], refs[chunks : chunks + plan.mates]
    far_ref, done_ref = refs[chunks + plan.mates :]
    room = chunks * plan.chunk
    me = plan.me()
    mine = plan.half(me)
    other = plan.partner(me)

    def scan(s, at):
        far_ref[s] = at
        near = (plan.half(s) == mine).astype(jnp.int32)
        return at + jnp.maximum(table_ref[s, 0, other] - plan.slots, 0) * near

    total = lax.fori_loop(0, plan.devices, scan, 0)
    for c, dense_ref in enumerate(dense):

        def step(i, carry):
            rows = pl.ds(pl.multiple_of(i * plan.full, plan.full), plan.full)
            tail = None
            if plan.extra:
                lasts = [plan.chunk * plan.full + e * plan.chunk + i for e in range(plan.extra)]
                tail = [dense_ref[pl.ds(last, 1), :] for last in lasts]
                tail = jnp.concatenate(tail, axis=0) if plan.extra > 1 else tail[0]
            done = advanced(params_ref, dense_ref[rows, :], tail)
            slot = c * plan.chunk + i
            to = pl.ds(pl.multiple_of(slot * plan.full, plan.full), plan.full)
            done_ref[to, :] = done[0]
            for e in range(plan.extra):
                row = room * plan.full + e * room + slot
                done_ref[pl.ds(row, 1), :] = done[1][e : e + 1]
            return carry

        lax.fori_loop(0, jnp.clip(total - c * plan.chunk, 0, plan.chunk), step, 0)
    here = plan.mate(me)
    slots = plan.over
    for d, out_ref in enumerate(outs):
        at = far_ref[plan.device(here ^ d, mine)]
        for k in range(slots):
            slot = jnp.minimum(at + k, room - 1)
            out_ref[k * plan.full : (k + 1) * plan.full, :] = done_ref[
                pl.ds(pl.multiple_of(slot * plan.full, plan.full), plan.full), :
            ]
            for e in range(plan.extra):
                row = slots * plan.full + e * slots + k
                out_ref[row : row + 1, :] = done_ref[
                    pl.ds(room * plan.full + e * room + slot, 1), :
                ]


def relay(plan, table, params, dense):
    piece = jax.ShapeDtypeStruct((plan.relay_rows, plan.width), dense[0].dtype)
    rows = round_up(len(dense) * plan.chunk * plan.rows, sublanes)
    return pl.pallas_call(
        functools.partial(relay_kernel, plan=plan, chunks=len(dense)),
        in_specs=[smem_full] + [vmem_full] * (1 + len(dense)),
        out_specs=[vmem_full] * plan.mates,
        out_shape=[piece] * plan.mates,
        scratch_shapes=[
            pltpu.SMEM((plan.devices,), jnp.int32),
            pltpu.VMEM((rows, plan.width), dense[0].dtype),
        ],
        name="relay",
    )(table, params, *dense)


def permuted(vals, lanes):
    return jnp.take_along_axis(vals, lanes, axis=1, mode="promise_in_bounds")


def unpack_kernel(base_ref, tail_ref, step_ref, perm_ref, *refs, plan, sizes):
    pieces = refs[: len(sizes)]
    out_ref, got_ref, last_ref, sem = refs[len(sizes) :]
    per_step, width = perm_ref.shape
    first = pl.program_id(0) * per_step

    @pl.when(first == 0)
    def _():
        copies, at = [], 0
        for i, (piece_ref, size) in enumerate(zip(pieces, sizes)):
            rows = pl.ds(at, size)
            copies.append(pltpu.make_async_copy(piece_ref, got_ref.at[rows], sem.at[i]))
            at += size
        for copy in copies:
            copy.start()
        for copy in copies:
            copy.wait()

    for i in range(per_step):
        base = pl.multiple_of(base_ref[first + i], sublanes)
        tail = tail_ref[first + i]
        stride = step_ref[first + i]
        lanes = jnp.broadcast_to(perm_ref[i : i + 1, :], (plan.full, width))
        vals = got_ref[pl.ds(base, plan.full), :]
        out_ref[0 : plan.full, i * width : (i + 1) * width] = permuted(vals, lanes)
        for e in range(plan.extra):
            last_ref[e, i : i + 1, :] = got_ref[pl.ds(tail + e * stride, 1), :]
    for e in range(plan.extra):
        last = permuted(last_ref[e], perm_ref[...])
        for i in range(per_step):
            cols = slice(i * width, (i + 1) * width)
            out_ref[plan.full + e : plan.full + e + 1, cols] = last[i : i + 1, :]


def unpack(plan, places, perm, pieces):
    per_step = fitting_blocks(plan.blocks, 16)
    sizes = [piece.shape[0] for piece in pieces]
    dtype = pieces[0].dtype
    return pl.pallas_call(
        functools.partial(unpack_kernel, plan=plan, sizes=sizes),
        grid_spec=pltpu.PrefetchScalarGridSpec(
            num_scalar_prefetch=3,
            grid=(plan.blocks // per_step,),
            in_specs=[pl.BlockSpec((per_step, plan.width), lambda i, *_: (i, 0))]
            + [any_full] * len(pieces),
            out_specs=pl.BlockSpec((plan.rows, per_step * plan.width), lambda i, *_: (0, i)),
            scratch_shapes=[
                pltpu.VMEM((sum(sizes), plan.width), dtype),
                pltpu.VMEM((max(plan.extra, 1), per_step, plan.width), dtype),
                pltpu.SemaphoreType.DMA((len(pieces),)),
            ],
        ),
        out_shape=jax.ShapeDtypeStruct((plan.rows, plan.blocks * plan.width), dtype),
        name="unpack",
    )(*places, perm, *pieces)


def fitting_blocks(total, most):
    size = min(total, most)
    while total % size:
        size -= 1
    return size


def find_places(plan, block_part, me):
    same = block_part[:, None] == block_part[None, :]
    position = jnp.arange(plan.blocks, dtype=jnp.int32)
    ahead = position[None, :] < position[:, None]
    rank = jnp.sum((same & ahead).astype(jnp.int32), axis=1, dtype=jnp.int32)
    home = plan.half(block_part) == plan.half(me)
    direct = rank < plan.slots
    piece = plan.mate(block_part) ^ plan.mate(me)
    crossed = plan.mates * plan.inner_rows + piece * plan.cross_rows
    relayed = plan.mates * (plan.inner_rows + plan.cross_rows) + piece * plan.relay_rows
    origin = jnp.where(home, piece * plan.inner_rows, jnp.where(direct, crossed, relayed))
    slots = jnp.where(home, plan.most, jnp.where(direct, plan.slots, plan.over))
    slot = jnp.where(home | direct, rank, rank - plan.slots)
    return origin + slot * plan.full, origin + slots * plan.full + slot, slots


def mixed(mates):
    pairs = [(d, mates - 1 - d) for d in range(mates // 2)]
    return [d for pair in pairs[1:] + pairs[:1] for d in pair]


def early_inner(mates):
    return [d for d in mixed(mates) if d][: mates // 2 - 1]


def exchange(plan, chunks, table, states, params, places, tile_perm):
    over = range(plan.devices)
    ends = {"inner": plan.half, "again": plan.half, "cross": lambda i: 1 - plan.half(i)}

    def send(kind, d, piece):
        pairs = [(i, plan.device(plan.mate(i) ^ d, ends[kind](i))) for i in over]
        return lax.ppermute(piece, both, pairs)

    dense = pack_dense(plan, table, states, chunks)
    crossed = []
    for c in range(chunks):
        crossed.append(
            lax.ppermute(dense[c], both, [(i, plan.partner(i)) for i in over])
        )
    adv = advance(params, states)
    first = early_inner(plan.mates)
    second = [d for d in range(plan.mates) if d not in first]
    inner = dict(zip(first, pack_pieces(plan, table, adv, first, [])))
    more = pack_pieces(plan, table, adv, second, list(range(plan.mates)))
    inner.update(zip(second, more))
    cross = list(more[len(second) :])
    again = list(relay(plan, table, params, crossed))
    for d in range(plan.mates):
        cross[d] = send("cross", d, cross[d])
        if d:
            inner[d] = send("inner", d, inner[d])
            again[d] = send("again", d, again[d])
    inner = [inner[d] for d in range(plan.mates)]
    return unpack(plan, places, tile_perm, [*inner, *cross, *again])


def on_device(
    states, block_part, tile_perm, half_volt, steepness, gate_rate, conductance, reversal
):
    blocks, width = tile_perm.shape
    plan = Plan(states.shape[0], blocks, width)
    devices = plan.devices
    me = plan.me()
    ids = jnp.arange(devices, dtype=jnp.int32)
    onehot = (block_part[:, None] == ids[None, :]).astype(jnp.int32)
    counts = jnp.sum(onehot, axis=0, dtype=jnp.int32)
    told = jnp.broadcast_to(counts[None, None, :], (devices, 1, devices))
    table = lax.all_to_all(told, both, split_axis=0, concat_axis=0, tiled=True)
    params = gate_params(half_volt, steepness, gate_rate, conductance, reversal, width)
    far = plan.half(ids)[:, None] != plan.half(ids)[None, :]
    spilled = jnp.maximum(table - plan.slots, 0)
    spilled = jnp.sum(jnp.where(far[:, None, :], spilled, 0), axis=0)
    spilled = jnp.max(spilled)
    places = find_places(plan, block_part, me)
    most = -(-plan.worst // plan.chunk)
    rooms = sorted({-(-most * 3 // 8), -(-most // 2), most})
    choice = sum((spilled > room * plan.chunk).astype(jnp.int32) for room in rooms[:-1])
    choice = jnp.asarray(choice, jnp.int32)
    return lax.switch(
        choice,
        [functools.partial(exchange, plan, room) for room in rooms],
        table,
        states,
        params,
        places,
        tile_perm,
    )


def solution(mesh):
    return jax.shard_map(
        on_device,
        mesh=mesh,
        in_specs=(
            P(None, both),
            P(both),
            P(both, None),
            P(),
            P(),
            P(),
            P(),
            P(),
        ),
        out_specs=P(None, both),
        check_vma=False,
    )
```

```python
import functools

import jax
import jax.numpy as jnp
from jax import lax
from jax.experimental import pallas as pl
from jax.experimental.pallas import tpu as pltpu
from jax.sharding import PartitionSpec as P


time_step = 0.25
sublanes = 8
both = ("group", "peer")
smem_full = pl.BlockSpec(memory_space=pltpu.SMEM)
vmem_full = pl.BlockSpec(memory_space=pltpu.VMEM)
any_full = pl.BlockSpec(memory_space=pl.ANY)


def round_up(value, step):
    return -(-value // step) * step


class Plan:
    def __init__(self, rows, blocks, width):
        self.rows, self.blocks, self.width = rows, blocks, width
        self.peers = lax.axis_size("peer")
        self.devices = lax.axis_size("group") * self.peers
        self.near = self.peers // 2
        self.mates = self.devices // 2
        most = 2 * blocks // self.devices
        self.slots = max(most // 2, 1)
        self.over = most - self.slots
        self.full = rows // sublanes * sublanes
        self.extra = rows - self.full
        self.most = self.slots + self.over
        self.inner_rows = round_up(rows * self.most, sublanes)
        self.cross_rows = round_up(rows * self.slots, sublanes)
        self.relay_rows = round_up(rows * self.over, sublanes)
        self.chunk = 16
        self.chunk_rows = round_up(rows * self.chunk, sublanes)
        self.worst = self.mates * self.over

    def half(self, device):
        return (device % self.peers) // self.near

    def mate(self, device):
        return device // self.peers * self.near + device % self.near

    def device(self, mate, half):
        return mate // self.near * self.peers + half * self.near + mate % self.near

    def partner(self, device):
        flip = 1 - 2 * self.half(device)
        return device + flip * self.near

    def me(self):
        return lax.axis_index("group") * self.peers + lax.axis_index("peer")


def advanced(params_ref, vals, tail):
    full = vals.shape[0]
    voltage = vals[0:1]
    relax = 1.5 + 0.5 * jnp.tanh(0.5 * voltage)
    done, current = [], 0.0
    for part, rows in ((vals, slice(0, full)), (tail, slice(full, None))):
        if part is None:
            continue
        steady = 0.5 + 0.5 * jnp.tanh((voltage - params_ref[0, rows]) * params_ref[1, rows])
        damping = jnp.exp(params_ref[2, rows] * relax)
        gates = steady + (part - steady) * damping
        drive = params_ref[3, rows] * gates * (voltage - params_ref[4, rows])
        current = current + jnp.sum(drive, axis=0, keepdims=True)
        done.append(gates)
    row = lax.broadcasted_iota(jnp.int32, vals.shape, 0)
    done[0] = jnp.where(row == 0, voltage - time_step * current, done[0])
    return done


def advance_kernel(params_ref, states_ref, out_ref, *, width):
    rows = states_ref.shape[0]
    full = rows // sublanes * sublanes

    lanes = 4 * width if states_ref.shape[1] % (4 * width) == 0 else width

    def one(i, carry):
        for j in range(lanes // width):
            at = pl.multiple_of(i * lanes + j * width, width)
            cols = pl.ds(at, width)
            tail = states_ref[full:rows, cols] if rows > full else None
            done = advanced(params_ref, states_ref[0:full, cols], tail)
            out_ref[0:full, cols] = done[0]
            if rows > full:
                out_ref[full:rows, cols] = done[1]
        return carry

    lax.fori_loop(0, states_ref.shape[1] // lanes, one, 0)


def gate_params(half_volt, steepness, gate_rate, conductance, reversal, width):
    params = jnp.stack([half_volt, 0.5 * steepness, -gate_rate, conductance, reversal])
    params = jnp.pad(params, ((0, 0), (1, 0)))
    return jnp.broadcast_to(params[:, :, None], params.shape + (width,))


def advance(params, states):
    rows, nodes = states.shape
    width = params.shape[2]
    block = fitting(nodes, 4096)
    return pl.pallas_call(
        functools.partial(advance_kernel, width=width),
        grid=(nodes // block,),
        in_specs=[
            pl.BlockSpec(params.shape, lambda i: (0, 0, 0)),
            pl.BlockSpec((rows, block), lambda i: (0, i)),
        ],
        out_specs=pl.BlockSpec((rows, block), lambda i: (0, i)),
        out_shape=jax.ShapeDtypeStruct(states.shape, states.dtype),
        cost_estimate=pl.CostEstimate(
            flops=40 * rows * nodes,
            bytes_accessed=8 * rows * nodes,
            transcendentals=3 * rows * nodes,
        ),
        name="advance",
    )(params, states)


def fitting(total, most):
    size = min(total, most)
    while total % size:
        size -= 128
    return size


def put_block(plan, adv_ref, block, put, base, tail):
    cols = pl.ds(pl.multiple_of(block * plan.width, plan.width), plan.width)
    put(base, plan.full, adv_ref[0 : plan.full, cols])
    for e in range(plan.extra):
        put(tail(e), 1, adv_ref[plan.full + e : plan.full + e + 1, cols])


def dense_kernel(table_ref, states_ref, *refs, plan):
    outs, all_ref = refs[:-1], refs[-1]
    room = len(outs) * plan.chunk
    me = plan.me()
    mine = plan.half(me)

    def one(s, carry):
        start, at = carry
        count = table_ref[s, 0, me]
        far = (plan.half(s) != mine).astype(jnp.int32)
        more = jnp.maximum(count - plan.slots, 0) * far

        def spill(k, carry):
            slot = jnp.minimum(at + k, room - 1)

            def put(base, size, vals):
                if size == plan.full:
                    base = pl.multiple_of(base, sublanes)
                all_ref[pl.ds(base, size), :] = vals

            put_block(
                plan,
                states_ref,
                start + plan.slots + k,
                put,
                slot * plan.full,
                lambda e: room * plan.full + e * room + slot,
            )
            return carry

        lax.fori_loop(0, more, spill, 0)
        return start + count, at + more

    lax.fori_loop(0, plan.devices, one, (0, 0))
    for c, out_ref in enumerate(outs):
        size = plan.chunk * plan.full
        out_ref[0:size, :] = all_ref[c * size : (c + 1) * size, :]
        for e in range(plan.extra):
            row = room * plan.full + e * room + c * plan.chunk
            to = size + e * plan.chunk
            out_ref[to : to + plan.chunk, :] = all_ref[row : row + plan.chunk, :]


def pack_dense(plan, table, states, chunks):
    piece = jax.ShapeDtypeStruct((plan.chunk_rows, plan.width), states.dtype)
    rows = round_up(chunks * plan.chunk * plan.rows, sublanes)
    return pl.pallas_call(
        functools.partial(dense_kernel, plan=plan),
        in_specs=[smem_full, vmem_full],
        out_specs=[vmem_full] * chunks,
        out_shape=[piece] * chunks,
        scratch_shapes=[pltpu.VMEM((rows, plan.width), states.dtype)],
        name="pack_dense",
    )(table, states)


def pieces_kernel(table_ref, adv_ref, *refs, plan, inner, cross):
    outs, start_ref = refs[:-1], refs[-1]
    me = plan.me()
    mine = plan.half(me)
    here = plan.mate(me)

    def scan(s, start):
        start_ref[s] = start
        return start + table_ref[s, 0, me]

    lax.fori_loop(0, plan.devices, scan, 0)
    jobs = [(d, mine, plan.most) for d in inner] + [(d, 1 - mine, plan.slots) for d in cross]
    for (d, half, slots), out_ref in zip(jobs, outs):
        start = start_ref[plan.device(here ^ d, half)]

        def put(base, size, vals):
            out_ref[base : base + size, :] = vals

        for k in range(slots):
            put_block(
                plan,
                adv_ref,
                jnp.minimum(start + k, plan.blocks - 1),
                put,
                k * plan.full,
                lambda e: slots * plan.full + e * slots + k,
            )


def pack_pieces(plan, table, adv, inner, cross):
    rows = [plan.inner_rows] * len(inner) + [plan.cross_rows] * len(cross)
    return pl.pallas_call(
        functools.partial(pieces_kernel, plan=plan, inner=inner, cross=cross),
        in_specs=[smem_full, vmem_full],
        out_specs=[vmem_full] * len(rows),
        out_shape=[jax.ShapeDtypeStruct((size, plan.width), adv.dtype) for size in rows],
        scratch_shapes=[pltpu.SMEM((plan.devices,), jnp.int32)],
    )(table, adv)


def relay_kernel(table_ref, params_ref, *refs, plan, chunks):
    dense, outs = refs[:chunks], refs[chunks : chunks + plan.mates]
    far_ref, done_ref = refs[chunks + plan.mates :]
    room = chunks * plan.chunk
    me = plan.me()
    mine = plan.half(me)
    other = plan.partner(me)

    def scan(s, at):
        far_ref[s] = at
        near = (plan.half(s) == mine).astype(jnp.int32)
        return at + jnp.maximum(table_ref[s, 0, other] - plan.slots, 0) * near

    total = lax.fori_loop(0, plan.devices, scan, 0)
    for c, dense_ref in enumerate(dense):

        def step(i, carry):
            rows = pl.ds(pl.multiple_of(i * plan.full, plan.full), plan.full)
            tail = None
            if plan.extra:
                lasts = [plan.chunk * plan.full + e * plan.chunk + i for e in range(plan.extra)]
                tail = [dense_ref[pl.ds(last, 1), :] for last in lasts]
                tail = jnp.concatenate(tail, axis=0) if plan.extra > 1 else tail[0]
            done = advanced(params_ref, dense_ref[rows, :], tail)
            slot = c * plan.chunk + i
            to = pl.ds(pl.multiple_of(slot * plan.full, plan.full), plan.full)
            done_ref[to, :] = done[0]
            for e in range(plan.extra):
                row = room * plan.full + e * room + slot
                done_ref[pl.ds(row, 1), :] = done[1][e : e + 1]
            return carry

        lax.fori_loop(0, jnp.clip(total - c * plan.chunk, 0, plan.chunk), step, 0)
    here = plan.mate(me)
    slots = plan.over
    for d, out_ref in enumerate(outs):
        at = far_ref[plan.device(here ^ d, mine)]
        for k in range(slots):
            slot = jnp.minimum(at + k, room - 1)
            out_ref[k * plan.full : (k + 1) * plan.full, :] = done_ref[
                pl.ds(pl.multiple_of(slot * plan.full, plan.full), plan.full), :
            ]
            for e in range(plan.extra):
                row = slots * plan.full + e * slots + k
                out_ref[row : row + 1, :] = done_ref[
                    pl.ds(room * plan.full + e * room + slot, 1), :
                ]


def relay(plan, table, params, dense):
    piece = jax.ShapeDtypeStruct((plan.relay_rows, plan.width), dense[0].dtype)
    rows = round_up(len(dense) * plan.chunk * plan.rows, sublanes)
    return pl.pallas_call(
        functools.partial(relay_kernel, plan=plan, chunks=len(dense)),
        in_specs=[smem_full] + [vmem_full] * (1 + len(dense)),
        out_specs=[vmem_full] * plan.mates,
        out_shape=[piece] * plan.mates,
        scratch_shapes=[
            pltpu.SMEM((plan.devices,), jnp.int32),
            pltpu.VMEM((rows, plan.width), dense[0].dtype),
        ],
        name="relay",
    )(table, params, *dense)


def permuted(vals, lanes):
    return jnp.take_along_axis(vals, lanes, axis=1, mode="promise_in_bounds")


def unpack_kernel(base_ref, tail_ref, step_ref, perm_ref, *refs, plan, sizes):
    pieces = refs[: len(sizes)]
    out_ref, got_ref, last_ref, sem = refs[len(sizes) :]
    per_step, width = perm_ref.shape
    first = pl.program_id(0) * per_step

    @pl.when(first == 0)
    def _():
        copies, at = [], 0
        for i, (piece_ref, size) in enumerate(zip(pieces, sizes)):
            rows = pl.ds(at, size)
            copies.append(pltpu.make_async_copy(piece_ref, got_ref.at[rows], sem.at[i]))
            at += size
        for copy in copies:
            copy.start()
        for copy in copies:
            copy.wait()

    for i in range(per_step):
        base = pl.multiple_of(base_ref[first + i], sublanes)
        tail = tail_ref[first + i]
        stride = step_ref[first + i]
        lanes = jnp.broadcast_to(perm_ref[i : i + 1, :], (plan.full, width))
        vals = got_ref[pl.ds(base, plan.full), :]
        out_ref[0 : plan.full, i * width : (i + 1) * width] = permuted(vals, lanes)
        for e in range(plan.extra):
            last_ref[e, i : i + 1, :] = got_ref[pl.ds(tail + e * stride, 1), :]
    for e in range(plan.extra):
        last = permuted(last_ref[e], perm_ref[...])
        for i in range(per_step):
            cols = slice(i * width, (i + 1) * width)
            out_ref[plan.full + e : plan.full + e + 1, cols] = last[i : i + 1, :]


def unpack(plan, places, perm, pieces):
    per_step = fitting_blocks(plan.blocks, 16)
    sizes = [piece.shape[0] for piece in pieces]
    dtype = pieces[0].dtype
    return pl.pallas_call(
        functools.partial(unpack_kernel, plan=plan, sizes=sizes),
        grid_spec=pltpu.PrefetchScalarGridSpec(
            num_scalar_prefetch=3,
            grid=(plan.blocks // per_step,),
            in_specs=[pl.BlockSpec((per_step, plan.width), lambda i, *_: (i, 0))]
            + [any_full] * len(pieces),
            out_specs=pl.BlockSpec((plan.rows, per_step * plan.width), lambda i, *_: (0, i)),
            scratch_shapes=[
                pltpu.VMEM((sum(sizes), plan.width), dtype),
                pltpu.VMEM((max(plan.extra, 1), per_step, plan.width), dtype),
                pltpu.SemaphoreType.DMA((len(pieces),)),
            ],
        ),
        out_shape=jax.ShapeDtypeStruct((plan.rows, plan.blocks * plan.width), dtype),
        name="unpack",
    )(*places, perm, *pieces)


def fitting_blocks(total, most):
    size = min(total, most)
    while total % size:
        size -= 1
    return size


def find_places(plan, block_part, me):
    same = block_part[:, None] == block_part[None, :]
    position = jnp.arange(plan.blocks, dtype=jnp.int32)
    ahead = position[None, :] < position[:, None]
    rank = jnp.sum((same & ahead).astype(jnp.int32), axis=1, dtype=jnp.int32)
    home = plan.half(block_part) == plan.half(me)
    direct = rank < plan.slots
    piece = plan.mate(block_part) ^ plan.mate(me)
    crossed = plan.mates * plan.inner_rows + piece * plan.cross_rows
    relayed = plan.mates * (plan.inner_rows + plan.cross_rows) + piece * plan.relay_rows
    origin = jnp.where(home, piece * plan.inner_rows, jnp.where(direct, crossed, relayed))
    slots = jnp.where(home, plan.most, jnp.where(direct, plan.slots, plan.over))
    slot = jnp.where(home | direct, rank, rank - plan.slots)
    return origin + slot * plan.full, origin + slots * plan.full + slot, slots


def mixed(mates):
    pairs = [(d, mates - 1 - d) for d in range(mates // 2)]
    return [d for pair in pairs[1:] + pairs[:1] for d in pair]


def early_inner(mates):
    return [d for d in mixed(mates) if d][: mates // 4]


def exchange(plan, chunks, table, states, params, places, tile_perm):
    over = range(plan.devices)
    ends = {"inner": plan.half, "again": plan.half, "cross": lambda i: 1 - plan.half(i)}

    def send(kind, d, piece):
        pairs = [(i, plan.device(plan.mate(i) ^ d, ends[kind](i))) for i in over]
        return lax.ppermute(piece, both, pairs)

    dense = pack_dense(plan, table, states, chunks)
    crossed = []
    for c in range(chunks):
        crossed.append(
            lax.ppermute(dense[c], both, [(i, plan.partner(i)) for i in over])
        )
    adv = advance(params, states)
    first = early_inner(plan.mates)
    second = [d for d in range(plan.mates) if d not in first]
    inner = dict(zip(first, pack_pieces(plan, table, adv, first, [])))
    more = pack_pieces(plan, table, adv, second, list(range(plan.mates)))
    inner.update(zip(second, more))
    cross = list(more[len(second) :])
    again = list(relay(plan, table, params, crossed))
    for d in range(plan.mates):
        cross[d] = send("cross", d, cross[d])
        if d:
            inner[d] = send("inner", d, inner[d])
            again[d] = send("again", d, again[d])
    inner = [inner[d] for d in range(plan.mates)]
    return unpack(plan, places, tile_perm, [*inner, *cross, *again])


def on_device(
    states, block_part, tile_perm, half_volt, steepness, gate_rate, conductance, reversal
):
    blocks, width = tile_perm.shape
    plan = Plan(states.shape[0], blocks, width)
    devices = plan.devices
    me = plan.me()
    ids = jnp.arange(devices, dtype=jnp.int32)
    onehot = (block_part[:, None] == ids[None, :]).astype(jnp.int32)
    counts = jnp.sum(onehot, axis=0, dtype=jnp.int32)
    told = jnp.broadcast_to(counts[None, None, :], (devices, 1, devices))
    table = lax.all_to_all(told, both, split_axis=0, concat_axis=0, tiled=True)
    params = gate_params(half_volt, steepness, gate_rate, conductance, reversal, width)
    far = plan.half(ids)[:, None] != plan.half(ids)[None, :]
    spilled = jnp.maximum(table - plan.slots, 0)
    spilled = jnp.sum(jnp.where(far[:, None, :], spilled, 0), axis=0)
    spilled = jnp.max(spilled)
    places = find_places(plan, block_part, me)
    most = -(-plan.worst // plan.chunk)
    rooms = sorted({-(-most * 3 // 8), -(-most // 2), most})
    choice = sum((spilled > room * plan.chunk).astype(jnp.int32) for room in rooms[:-1])
    choice = jnp.asarray(choice, jnp.int32)
    return lax.switch(
        choice,
        [functools.partial(exchange, plan, room) for room in rooms],
        table,
        states,
        params,
        places,
        tile_perm,
    )


def solution(mesh):
    return jax.shard_map(
        on_device,
        mesh=mesh,
        in_specs=(
            P(None, both),
            P(both),
            P(both, None),
            P(),
            P(),
            P(),
            P(),
            P(),
        ),
        out_specs=P(None, both),
        check_vma=False,
    )
```

```python
import functools

import jax
import jax.numpy as jnp
from jax import lax
from jax.experimental import pallas as pl
from jax.experimental.pallas import tpu as pltpu
from jax.sharding import PartitionSpec as P


time_step = 0.25
sublanes = 8
both = ("group", "peer")
smem_full = pl.BlockSpec(memory_space=pltpu.SMEM)
vmem_full = pl.BlockSpec(memory_space=pltpu.VMEM)
any_full = pl.BlockSpec(memory_space=pl.ANY)


def round_up(value, step):
    return -(-value // step) * step


class Plan:
    def __init__(self, rows, blocks, width):
        self.rows, self.blocks, self.width = rows, blocks, width
        self.peers = lax.axis_size("peer")
        self.devices = lax.axis_size("group") * self.peers
        self.near = self.peers // 2
        self.mates = self.devices // 2
        most = 2 * blocks // self.devices
        self.slots = max(most // 2, 1)
        self.over = most - self.slots
        self.full = rows // sublanes * sublanes
        self.extra = rows - self.full
        self.most = self.slots + self.over
        self.inner_rows = round_up(rows * self.most, sublanes)
        self.cross_rows = round_up(rows * self.slots, sublanes)
        self.relay_rows = round_up(rows * 2 * self.over, sublanes)
        self.side = self.peers // 4
        self.flat = self.devices // 4
        self.worst = self.flat * self.over

    def half(self, device):
        return (device % self.peers) // self.near

    def mate(self, device):
        return device // self.peers * self.near + device % self.near

    def device(self, mate, half):
        return mate // self.near * self.peers + half * self.near + mate % self.near

    def plane(self, device):
        return device % self.peers // self.side

    def spot(self, device):
        return device // self.peers * self.side + device % self.side

    def at(self, spot, plane):
        return spot // self.side * self.peers + plane * self.side + spot % self.side

    def twin(self, device, flip):
        return self.at(self.spot(device), self.plane(device) ^ flip)

    def me(self):
        return lax.axis_index("group") * self.peers + lax.axis_index("peer")


def advanced(params_ref, vals, tail):
    full = vals.shape[0]
    voltage = vals[0:1]
    relax = 1.5 + 0.5 * jnp.tanh(0.5 * voltage)
    done, current = [], 0.0
    for part, rows in ((vals, slice(0, full)), (tail, slice(full, None))):
        if part is None:
            continue
        steady = 0.5 + 0.5 * jnp.tanh((voltage - params_ref[0, rows]) * params_ref[1, rows])
        damping = jnp.exp(params_ref[2, rows] * relax)
        gates = steady + (part - steady) * damping
        drive = params_ref[3, rows] * gates * (voltage - params_ref[4, rows])
        current = current + jnp.sum(drive, axis=0, keepdims=True)
        done.append(gates)
    row = lax.broadcasted_iota(jnp.int32, vals.shape, 0)
    done[0] = jnp.where(row == 0, voltage - time_step * current, done[0])
    return done


def advance_kernel(params_ref, states_ref, out_ref, *, width):
    rows = states_ref.shape[0]
    full = rows // sublanes * sublanes

    lanes = 4 * width if states_ref.shape[1] % (4 * width) == 0 else width

    def one(i, carry):
        for j in range(lanes // width):
            at = pl.multiple_of(i * lanes + j * width, width)
            cols = pl.ds(at, width)
            tail = states_ref[full:rows, cols] if rows > full else None
            done = advanced(params_ref, states_ref[0:full, cols], tail)
            out_ref[0:full, cols] = done[0]
            if rows > full:
                out_ref[full:rows, cols] = done[1]
        return carry

    lax.fori_loop(0, states_ref.shape[1] // lanes, one, 0)


def gate_params(half_volt, steepness, gate_rate, conductance, reversal, width):
    params = jnp.stack([half_volt, 0.5 * steepness, -gate_rate, conductance, reversal])
    params = jnp.pad(params, ((0, 0), (1, 0)))
    return jnp.broadcast_to(params[:, :, None], params.shape + (width,))


def advance(params, states):
    rows, nodes = states.shape
    width = params.shape[2]
    block = fitting(nodes, 4096)
    return pl.pallas_call(
        functools.partial(advance_kernel, width=width),
        grid=(nodes // block,),
        in_specs=[
            pl.BlockSpec(params.shape, lambda i: (0, 0, 0)),
            pl.BlockSpec((rows, block), lambda i: (0, i)),
        ],
        out_specs=pl.BlockSpec((rows, block), lambda i: (0, i)),
        out_shape=jax.ShapeDtypeStruct(states.shape, states.dtype),
        cost_estimate=pl.CostEstimate(
            flops=40 * rows * nodes,
            bytes_accessed=8 * rows * nodes,
            transcendentals=3 * rows * nodes,
        ),
        name="advance",
    )(params, states)


def fitting(total, most):
    size = min(total, most)
    while total % size:
        size -= 128
    return size


def put_block(plan, adv_ref, block, put, base, tail):
    cols = pl.ds(pl.multiple_of(block * plan.width, plan.width), plan.width)
    put(base, plan.full, adv_ref[0 : plan.full, cols])
    for e in range(plan.extra):
        put(tail(e), 1, adv_ref[plan.full + e : plan.full + e + 1, cols])


far_planes = (2, 3)


def dense_kernel(table_ref, states_ref, *outs, plan, room):
    me = plan.me()

    def one(s, carry):
        start, *places = carry
        count = table_ref[s, 0, me]
        flip = plan.plane(s) ^ plan.plane(me)
        spilled = jnp.maximum(count - plan.slots, 0)
        nexts = []
        for far, at, out_ref in zip(far_planes, places, outs):
            more = spilled * (flip == far).astype(jnp.int32)

            def spill(k, carry, at=at, out_ref=out_ref):
                slot = jnp.minimum(at + k, room - 1)

                def put(base, size, vals):
                    if size == plan.full:
                        base = pl.multiple_of(base, sublanes)
                    out_ref[pl.ds(base, size), :] = vals

                put_block(
                    plan,
                    states_ref,
                    start + plan.slots + k,
                    put,
                    slot * plan.full,
                    lambda e: room * plan.full + e * room + slot,
                )
                return carry

            lax.fori_loop(0, more, spill, 0)
            nexts.append(at + more)
        return (start + count, *nexts)

    lax.fori_loop(0, plan.devices, one, (0, 0, 0))


def pack_dense(plan, table, states, room):
    rows = round_up(room * plan.rows, sublanes)
    piece = jax.ShapeDtypeStruct((rows, plan.width), states.dtype)
    return pl.pallas_call(
        functools.partial(dense_kernel, plan=plan, room=room),
        in_specs=[smem_full, vmem_full],
        out_specs=[vmem_full] * 2,
        out_shape=[piece] * 2,
        name="pack_dense",
    )(table, states)


def pieces_kernel(table_ref, adv_ref, *refs, plan, inner, cross):
    outs, start_ref = refs[:-1], refs[-1]
    me = plan.me()
    mine = plan.half(me)
    here = plan.mate(me)

    def scan(s, start):
        start_ref[s] = start
        return start + table_ref[s, 0, me]

    lax.fori_loop(0, plan.devices, scan, 0)
    jobs = [(d, mine, plan.most) for d in inner] + [(d, 1 - mine, plan.slots) for d in cross]
    for (d, half, slots), out_ref in zip(jobs, outs):
        start = start_ref[plan.device(here ^ d, half)]

        def put(base, size, vals):
            out_ref[base : base + size, :] = vals

        for k in range(slots):
            put_block(
                plan,
                adv_ref,
                jnp.minimum(start + k, plan.blocks - 1),
                put,
                k * plan.full,
                lambda e: slots * plan.full + e * slots + k,
            )


def pack_pieces(plan, table, adv, inner, cross):
    rows = [plan.inner_rows] * len(inner) + [plan.cross_rows] * len(cross)
    return pl.pallas_call(
        functools.partial(pieces_kernel, plan=plan, inner=inner, cross=cross),
        in_specs=[smem_full, vmem_full],
        out_specs=[vmem_full] * len(rows),
        out_shape=[jax.ShapeDtypeStruct((size, plan.width), adv.dtype) for size in rows],
        scratch_shapes=[pltpu.SMEM((plan.devices,), jnp.int32)],
    )(table, adv)


def relay_kernel(table_ref, params_ref, *refs, plan, room):
    dense, outs = refs[:2], refs[2 : 2 + plan.flat]
    first_refs, done_refs = refs[2 + plan.flat : 4 + plan.flat], refs[4 + plan.flat :]
    me = plan.me()
    plane = plan.plane(me)
    here = plan.spot(me)
    slots = 2 * plan.over
    for j, far in enumerate(far_planes):
        dense_ref, done_ref, first_ref = dense[j], done_refs[j], first_refs[j]
        source = plan.twin(me, far)

        def scan(t, at):
            first_ref[t] = at
            return at + jnp.maximum(table_ref[plan.at(t, plane), 0, source] - plan.slots, 0)

        total = lax.fori_loop(0, plan.flat, scan, 0)

        def step(i, carry):
            rows = pl.ds(pl.multiple_of(i * plan.full, plan.full), plan.full)
            lasts = [pl.ds(room * plan.full + e * room + i, 1) for e in range(plan.extra)]
            tail = None
            if plan.extra:
                tail = [dense_ref[last, :] for last in lasts]
                tail = jnp.concatenate(tail, axis=0) if plan.extra > 1 else tail[0]
            done = advanced(params_ref, dense_ref[rows, :], tail)
            done_ref[rows, :] = done[0]
            for e, last in enumerate(lasts):
                done_ref[last, :] = done[1][e : e + 1]
            return carry

        lax.fori_loop(0, jnp.minimum(total, room), step, 0)
        for d, out_ref in enumerate(outs):
            at = first_ref[here ^ d]
            for k in range(plan.over):
                slot = jnp.minimum(at + k, room - 1)
                to = j * plan.over + k
                out_ref[to * plan.full : (to + 1) * plan.full, :] = done_ref[
                    pl.ds(pl.multiple_of(slot * plan.full, plan.full), plan.full), :
                ]
                for e in range(plan.extra):
                    row = slots * plan.full + e * slots + to
                    out_ref[row : row + 1, :] = done_ref[
                        pl.ds(room * plan.full + e * room + slot, 1), :
                    ]


def relay(plan, table, params, dense, room):
    piece = jax.ShapeDtypeStruct((plan.relay_rows, plan.width), dense[0].dtype)
    starts = pltpu.SMEM((plan.flat,), jnp.int32)
    blocks = pltpu.VMEM(dense[0].shape, dense[0].dtype)
    return pl.pallas_call(
        functools.partial(relay_kernel, plan=plan, room=room),
        in_specs=[smem_full] + [vmem_full] * 3,
        out_specs=[vmem_full] * plan.flat,
        out_shape=[piece] * plan.flat,
        scratch_shapes=[starts, starts, blocks, blocks],
        name="relay",
    )(table, params, *dense)


def permuted(vals, lanes):
    return jnp.take_along_axis(vals, lanes, axis=1, mode="promise_in_bounds")


def unpack_kernel(base_ref, tail_ref, step_ref, perm_ref, *refs, plan, sizes):
    pieces = refs[: len(sizes)]
    out_ref, got_ref, last_ref, sem = refs[len(sizes) :]
    per_step, width = perm_ref.shape
    first = pl.program_id(0) * per_step

    @pl.when(first == 0)
    def _():
        copies, at = [], 0
        for i, (piece_ref, size) in enumerate(zip(pieces, sizes)):
            rows = pl.ds(at, size)
            copies.append(pltpu.make_async_copy(piece_ref, got_ref.at[rows], sem.at[i]))
            at += size
        for copy in copies:
            copy.start()
        for copy in copies:
            copy.wait()

    for i in range(per_step):
        base = pl.multiple_of(base_ref[first + i], sublanes)
        tail = tail_ref[first + i]
        stride = step_ref[first + i]
        lanes = jnp.broadcast_to(perm_ref[i : i + 1, :], (plan.full, width))
        vals = got_ref[pl.ds(base, plan.full), :]
        out_ref[0 : plan.full, i * width : (i + 1) * width] = permuted(vals, lanes)
        for e in range(plan.extra):
            last_ref[e, i : i + 1, :] = got_ref[pl.ds(tail + e * stride, 1), :]
    for e in range(plan.extra):
        last = permuted(last_ref[e], perm_ref[...])
        for i in range(per_step):
            cols = slice(i * width, (i + 1) * width)
            out_ref[plan.full + e : plan.full + e + 1, cols] = last[i : i + 1, :]


def unpack(plan, places, perm, pieces):
    per_step = fitting_blocks(plan.blocks, 16)
    sizes = [piece.shape[0] for piece in pieces]
    dtype = pieces[0].dtype
    return pl.pallas_call(
        functools.partial(unpack_kernel, plan=plan, sizes=sizes),
        grid_spec=pltpu.PrefetchScalarGridSpec(
            num_scalar_prefetch=3,
            grid=(plan.blocks // per_step,),
            in_specs=[pl.BlockSpec((per_step, plan.width), lambda i, *_: (i, 0))]
            + [any_full] * len(pieces),
            out_specs=pl.BlockSpec((plan.rows, per_step * plan.width), lambda i, *_: (0, i)),
            scratch_shapes=[
                pltpu.VMEM((sum(sizes), plan.width), dtype),
                pltpu.VMEM((max(plan.extra, 1), per_step, plan.width), dtype),
                pltpu.SemaphoreType.DMA((len(pieces),)),
            ],
        ),
        out_shape=jax.ShapeDtypeStruct((plan.rows, plan.blocks * plan.width), dtype),
        name="unpack",
    )(*places, perm, *pieces)


def fitting_blocks(total, most):
    size = min(total, most)
    while total % size:
        size -= 1
    return size


def find_places(plan, block_part, me):
    same = block_part[:, None] == block_part[None, :]
    position = jnp.arange(plan.blocks, dtype=jnp.int32)
    ahead = position[None, :] < position[:, None]
    rank = jnp.sum((same & ahead).astype(jnp.int32), axis=1, dtype=jnp.int32)
    home = plan.half(block_part) == plan.half(me)
    direct = rank < plan.slots
    piece = plan.mate(block_part) ^ plan.mate(me)
    crossed = plan.mates * plan.inner_rows + piece * plan.cross_rows
    spot = plan.spot(block_part) ^ plan.spot(me)
    relayed = plan.mates * (plan.inner_rows + plan.cross_rows) + spot * plan.relay_rows
    origin = jnp.where(home, piece * plan.inner_rows, jnp.where(direct, crossed, relayed))
    slots = jnp.where(home, plan.most, jnp.where(direct, plan.slots, 2 * plan.over))
    flip = plan.plane(block_part) ^ plan.plane(me)
    shift = jnp.where(flip == far_planes[0], 0, plan.over) - plan.slots
    slot = jnp.where(home | direct, rank, rank + shift)
    return origin + slot * plan.full, origin + slots * plan.full + slot, slots


def mixed(mates):
    pairs = [(d, mates - 1 - d) for d in range(mates // 2)]
    return [d for pair in pairs[1:] + pairs[:1] for d in pair]


def early_inner(mates, side):
    across = [d for d in mixed(mates) if d & side]
    return across[: len(across) // 2]


def exchange(plan, room, table, states, params, places, tile_perm):
    over = range(plan.devices)

    def send(piece, target):
        return lax.ppermute(piece, both, [(i, target(i)) for i in over])

    dense = pack_dense(plan, table, states, room)
    crossed = [
        send(piece, functools.partial(plan.twin, flip=far))
        for far, piece in zip(far_planes, dense)
    ]
    adv = advance(params, states)
    first = early_inner(plan.mates, plan.side)
    second = [d for d in range(plan.mates) if d not in first]
    inner = dict(zip(first, pack_pieces(plan, table, adv, first, [])))
    more = pack_pieces(plan, table, adv, second, list(range(plan.mates)))
    inner.update(zip(second, more))
    cross = list(more[len(second) :])
    again = list(relay(plan, table, params, crossed, room))
    for d in range(plan.mates):
        cross[d] = send(cross[d], lambda i: plan.device(plan.mate(i) ^ d, 1 - plan.half(i)))
        if d:
            inner[d] = send(inner[d], lambda i: plan.device(plan.mate(i) ^ d, plan.half(i)))
    for d in range(1, plan.flat):
        again[d] = send(again[d], lambda i: plan.at(plan.spot(i) ^ d, plan.plane(i)))
    inner = [inner[d] for d in range(plan.mates)]
    return unpack(plan, places, tile_perm, [*inner, *cross, *again])


def on_device(
    states, block_part, tile_perm, half_volt, steepness, gate_rate, conductance, reversal
):
    blocks, width = tile_perm.shape
    plan = Plan(states.shape[0], blocks, width)
    devices = plan.devices
    me = plan.me()
    ids = jnp.arange(devices, dtype=jnp.int32)
    onehot = (block_part[:, None] == ids[None, :]).astype(jnp.int32)
    counts = jnp.sum(onehot, axis=0, dtype=jnp.int32)
    told = jnp.broadcast_to(counts[None, None, :], (devices, 1, devices))
    table = lax.all_to_all(told, both, split_axis=0, concat_axis=0, tiled=True)
    params = gate_params(half_volt, steepness, gate_rate, conductance, reversal, width)
    spilled = jnp.maximum(table[:, 0, :] - plan.slots, 0)
    planes = plan.plane(ids)
    across = plan.half(ids)[:, None] != plan.half(ids)[None, :]
    totals = [
        jnp.sum(jnp.where(across & (planes == q)[:, None], spilled, 0), axis=0)
        for q in range(4)
    ]
    spilled = jnp.max(jnp.stack(totals))
    places = find_places(plan, block_part, me)
    rooms = {round_up(plan.worst * eighths // 8, sublanes) for eighths in (3, 4, 5, 8)}
    rooms = sorted(rooms)
    choice = sum((spilled > room).astype(jnp.int32) for room in rooms[:-1])
    return lax.switch(
        choice,
        [functools.partial(exchange, plan, room) for room in rooms],
        table,
        states,
        params,
        places,
        tile_perm,
    )


def solution(mesh):
    return jax.shard_map(
        on_device,
        mesh=mesh,
        in_specs=(
            P(None, both),
            P(both),
            P(both, None),
            P(),
            P(),
            P(),
            P(),
            P(),
        ),
        out_specs=P(None, both),
        check_vma=False,
    )
```

```python
import functools

import jax
import jax.numpy as jnp
from jax import lax
from jax.experimental import pallas as pl
from jax.experimental.pallas import tpu as pltpu
from jax.sharding import PartitionSpec as P


time_step = 0.25
sublanes = 8
both = ("group", "peer")
smem_full = pl.BlockSpec(memory_space=pltpu.SMEM)
vmem_full = pl.BlockSpec(memory_space=pltpu.VMEM)
any_full = pl.BlockSpec(memory_space=pl.ANY)


def round_up(value, step):
    return -(-value // step) * step


class Plan:
    def __init__(self, rows, blocks, width):
        self.rows, self.blocks, self.width = rows, blocks, width
        self.peers = lax.axis_size("peer")
        self.devices = lax.axis_size("group") * self.peers
        self.near = self.peers // 2
        self.mates = self.devices // 2
        most = 2 * blocks // self.devices
        self.slots = max(3 * most // 8, 1)
        self.over = most - self.slots
        self.full = rows // sublanes * sublanes
        self.extra = rows - self.full
        self.most = self.slots + self.over
        self.inner_rows = round_up(rows * self.most, sublanes)
        self.cross_rows = round_up(rows * self.slots, sublanes)
        self.relay_rows = round_up(rows * 2 * self.over, sublanes)
        self.side = self.peers // 4
        self.flat = self.devices // 4
        self.worst = self.flat * self.over

    def half(self, device):
        return (device % self.peers) // self.near

    def mate(self, device):
        return device // self.peers * self.near + device % self.near

    def device(self, mate, half):
        return mate // self.near * self.peers + half * self.near + mate % self.near

    def plane(self, device):
        return device % self.peers // self.side

    def spot(self, device):
        return device // self.peers * self.side + device % self.side

    def at(self, spot, plane):
        return spot // self.side * self.peers + plane * self.side + spot % self.side

    def twin(self, device, flip):
        return self.at(self.spot(device), self.plane(device) ^ flip)

    def me(self):
        return lax.axis_index("group") * self.peers + lax.axis_index("peer")


def advanced(params_ref, vals, tail):
    full = vals.shape[0]
    voltage = vals[0:1]
    relax = 1.5 + 0.5 * jnp.tanh(0.5 * voltage)
    done, current = [], 0.0
    for part, rows in ((vals, slice(0, full)), (tail, slice(full, None))):
        if part is None:
            continue
        steady = 0.5 + 0.5 * jnp.tanh((voltage - params_ref[0, rows]) * params_ref[1, rows])
        damping = jnp.exp(params_ref[2, rows] * relax)
        gates = steady + (part - steady) * damping
        drive = params_ref[3, rows] * gates * (voltage - params_ref[4, rows])
        current = current + jnp.sum(drive, axis=0, keepdims=True)
        done.append(gates)
    row = lax.broadcasted_iota(jnp.int32, vals.shape, 0)
    done[0] = jnp.where(row == 0, voltage - time_step * current, done[0])
    return done


def advance_kernel(params_ref, states_ref, out_ref, *, width):
    rows = states_ref.shape[0]
    full = rows // sublanes * sublanes

    lanes = 4 * width if states_ref.shape[1] % (4 * width) == 0 else width

    def one(i, carry):
        for j in range(lanes // width):
            at = pl.multiple_of(i * lanes + j * width, width)
            cols = pl.ds(at, width)
            tail = states_ref[full:rows, cols] if rows > full else None
            done = advanced(params_ref, states_ref[0:full, cols], tail)
            out_ref[0:full, cols] = done[0]
            if rows > full:
                out_ref[full:rows, cols] = done[1]
        return carry

    lax.fori_loop(0, states_ref.shape[1] // lanes, one, 0)


def gate_params(half_volt, steepness, gate_rate, conductance, reversal, width):
    params = jnp.stack([half_volt, 0.5 * steepness, -gate_rate, conductance, reversal])
    params = jnp.pad(params, ((0, 0), (1, 0)))
    return jnp.broadcast_to(params[:, :, None], params.shape + (width,))


def advance(params, states):
    rows, nodes = states.shape
    width = params.shape[2]
    block = fitting(nodes, 4096)
    return pl.pallas_call(
        functools.partial(advance_kernel, width=width),
        grid=(nodes // block,),
        in_specs=[
            pl.BlockSpec(params.shape, lambda i: (0, 0, 0)),
            pl.BlockSpec((rows, block), lambda i: (0, i)),
        ],
        out_specs=pl.BlockSpec((rows, block), lambda i: (0, i)),
        out_shape=jax.ShapeDtypeStruct(states.shape, states.dtype),
        cost_estimate=pl.CostEstimate(
            flops=40 * rows * nodes,
            bytes_accessed=8 * rows * nodes,
            transcendentals=3 * rows * nodes,
        ),
        name="advance",
    )(params, states)


def fitting(total, most):
    size = min(total, most)
    while total % size:
        size -= 128
    return size


def put_block(plan, adv_ref, block, put, base, tail):
    cols = pl.ds(pl.multiple_of(block * plan.width, plan.width), plan.width)
    put(base, plan.full, adv_ref[0 : plan.full, cols])
    for e in range(plan.extra):
        put(tail(e), 1, adv_ref[plan.full + e : plan.full + e + 1, cols])


far_planes = (2, 3)


def dense_kernel(table_ref, states_ref, *outs, plan, room):
    me = plan.me()

    def one(s, carry):
        start, *places = carry
        count = table_ref[s, 0, me]
        flip = plan.plane(s) ^ plan.plane(me)
        spilled = jnp.maximum(count - plan.slots, 0)
        nexts = []
        for far, at, out_ref in zip(far_planes, places, outs):
            more = spilled * (flip == far).astype(jnp.int32)

            def spill(k, carry, at=at, out_ref=out_ref):
                slot = jnp.minimum(at + k, room - 1)

                def put(base, size, vals):
                    if size == plan.full:
                        base = pl.multiple_of(base, sublanes)
                    out_ref[pl.ds(base, size), :] = vals

                put_block(
                    plan,
                    states_ref,
                    start + plan.slots + k,
                    put,
                    slot * plan.full,
                    lambda e: room * plan.full + e * room + slot,
                )
                return carry

            lax.fori_loop(0, more, spill, 0)
            nexts.append(at + more)
        return (start + count, *nexts)

    lax.fori_loop(0, plan.devices, one, (0, 0, 0))


def pack_dense(plan, table, states, room):
    rows = round_up(room * plan.rows, sublanes)
    piece = jax.ShapeDtypeStruct((rows, plan.width), states.dtype)
    return pl.pallas_call(
        functools.partial(dense_kernel, plan=plan, room=room),
        in_specs=[smem_full, vmem_full],
        out_specs=[vmem_full] * 2,
        out_shape=[piece] * 2,
        name="pack_dense",
    )(table, states)


def pieces_kernel(table_ref, adv_ref, *refs, plan, inner, cross):
    outs, start_ref = refs[:-1], refs[-1]
    me = plan.me()
    mine = plan.half(me)
    here = plan.mate(me)

    def scan(s, start):
        start_ref[s] = start
        return start + table_ref[s, 0, me]

    lax.fori_loop(0, plan.devices, scan, 0)
    jobs = [(d, mine, plan.most) for d in inner] + [(d, 1 - mine, plan.slots) for d in cross]
    for (d, half, slots), out_ref in zip(jobs, outs):
        start = start_ref[plan.device(here ^ d, half)]

        def put(base, size, vals):
            out_ref[base : base + size, :] = vals

        for k in range(slots):
            put_block(
                plan,
                adv_ref,
                jnp.minimum(start + k, plan.blocks - 1),
                put,
                k * plan.full,
                lambda e: slots * plan.full + e * slots + k,
            )


def pack_pieces(plan, table, adv, inner, cross):
    rows = [plan.inner_rows] * len(inner) + [plan.cross_rows] * len(cross)
    return pl.pallas_call(
        functools.partial(pieces_kernel, plan=plan, inner=inner, cross=cross),
        in_specs=[smem_full, vmem_full],
        out_specs=[vmem_full] * len(rows),
        out_shape=[jax.ShapeDtypeStruct((size, plan.width), adv.dtype) for size in rows],
        scratch_shapes=[pltpu.SMEM((plan.devices,), jnp.int32)],
    )(table, adv)


def relay_kernel(table_ref, params_ref, *refs, plan, room):
    dense, outs = refs[:2], refs[2 : 2 + plan.flat]
    first_refs, done_refs = refs[2 + plan.flat : 4 + plan.flat], refs[4 + plan.flat :]
    me = plan.me()
    plane = plan.plane(me)
    here = plan.spot(me)
    slots = 2 * plan.over
    for j, far in enumerate(far_planes):
        dense_ref, done_ref, first_ref = dense[j], done_refs[j], first_refs[j]
        source = plan.twin(me, far)

        def scan(t, at):
            first_ref[t] = at
            return at + jnp.maximum(table_ref[plan.at(t, plane), 0, source] - plan.slots, 0)

        total = lax.fori_loop(0, plan.flat, scan, 0)

        def step(i, carry):
            rows = pl.ds(pl.multiple_of(i * plan.full, plan.full), plan.full)
            lasts = [pl.ds(room * plan.full + e * room + i, 1) for e in range(plan.extra)]
            tail = None
            if plan.extra:
                tail = [dense_ref[last, :] for last in lasts]
                tail = jnp.concatenate(tail, axis=0) if plan.extra > 1 else tail[0]
            done = advanced(params_ref, dense_ref[rows, :], tail)
            done_ref[rows, :] = done[0]
            for e, last in enumerate(lasts):
                done_ref[last, :] = done[1][e : e + 1]
            return carry

        lax.fori_loop(0, jnp.minimum(total, room), step, 0)
        for d, out_ref in enumerate(outs):
            at = first_ref[here ^ d]
            for k in range(plan.over):
                slot = jnp.minimum(at + k, room - 1)
                to = j * plan.over + k
                out_ref[to * plan.full : (to + 1) * plan.full, :] = done_ref[
                    pl.ds(pl.multiple_of(slot * plan.full, plan.full), plan.full), :
                ]
                for e in range(plan.extra):
                    row = slots * plan.full + e * slots + to
                    out_ref[row : row + 1, :] = done_ref[
                        pl.ds(room * plan.full + e * room + slot, 1), :
                    ]


def relay(plan, table, params, dense, room):
    piece = jax.ShapeDtypeStruct((plan.relay_rows, plan.width), dense[0].dtype)
    starts = pltpu.SMEM((plan.flat,), jnp.int32)
    blocks = pltpu.VMEM(dense[0].shape, dense[0].dtype)
    return pl.pallas_call(
        functools.partial(relay_kernel, plan=plan, room=room),
        in_specs=[smem_full] + [vmem_full] * 3,
        out_specs=[vmem_full] * plan.flat,
        out_shape=[piece] * plan.flat,
        scratch_shapes=[starts, starts, blocks, blocks],
        name="relay",
    )(table, params, *dense)


def permuted(vals, lanes):
    return jnp.take_along_axis(vals, lanes, axis=1, mode="promise_in_bounds")


def unpack_kernel(base_ref, tail_ref, step_ref, perm_ref, *refs, plan, sizes):
    pieces = refs[: len(sizes)]
    out_ref, got_ref, last_ref, sem = refs[len(sizes) :]
    per_step, width = perm_ref.shape
    first = pl.program_id(0) * per_step

    @pl.when(first == 0)
    def _():
        copies, at = [], 0
        for i, (piece_ref, size) in enumerate(zip(pieces, sizes)):
            rows = pl.ds(at, size)
            copies.append(pltpu.make_async_copy(piece_ref, got_ref.at[rows], sem.at[i]))
            at += size
        for copy in copies:
            copy.start()
        for copy in copies:
            copy.wait()

    for i in range(per_step):
        base = pl.multiple_of(base_ref[first + i], sublanes)
        tail = tail_ref[first + i]
        stride = step_ref[first + i]
        lanes = jnp.broadcast_to(perm_ref[i : i + 1, :], (plan.full, width))
        vals = got_ref[pl.ds(base, plan.full), :]
        out_ref[0 : plan.full, i * width : (i + 1) * width] = permuted(vals, lanes)
        for e in range(plan.extra):
            last_ref[e, i : i + 1, :] = got_ref[pl.ds(tail + e * stride, 1), :]
    for e in range(plan.extra):
        last = permuted(last_ref[e], perm_ref[...])
        for i in range(per_step):
            cols = slice(i * width, (i + 1) * width)
            out_ref[plan.full + e : plan.full + e + 1, cols] = last[i : i + 1, :]


def unpack(plan, places, perm, pieces):
    per_step = fitting_blocks(plan.blocks, 16)
    sizes = [piece.shape[0] for piece in pieces]
    dtype = pieces[0].dtype
    return pl.pallas_call(
        functools.partial(unpack_kernel, plan=plan, sizes=sizes),
        grid_spec=pltpu.PrefetchScalarGridSpec(
            num_scalar_prefetch=3,
            grid=(plan.blocks // per_step,),
            in_specs=[pl.BlockSpec((per_step, plan.width), lambda i, *_: (i, 0))]
            + [any_full] * len(pieces),
            out_specs=pl.BlockSpec((plan.rows, per_step * plan.width), lambda i, *_: (0, i)),
            scratch_shapes=[
                pltpu.VMEM((sum(sizes), plan.width), dtype),
                pltpu.VMEM((max(plan.extra, 1), per_step, plan.width), dtype),
                pltpu.SemaphoreType.DMA((len(pieces),)),
            ],
        ),
        out_shape=jax.ShapeDtypeStruct((plan.rows, plan.blocks * plan.width), dtype),
        name="unpack",
    )(*places, perm, *pieces)


def fitting_blocks(total, most):
    size = min(total, most)
    while total % size:
        size -= 1
    return size


def find_places(plan, block_part, me):
    same = block_part[:, None] == block_part[None, :]
    position = jnp.arange(plan.blocks, dtype=jnp.int32)
    ahead = position[None, :] < position[:, None]
    rank = jnp.sum((same & ahead).astype(jnp.int32), axis=1, dtype=jnp.int32)
    home = plan.half(block_part) == plan.half(me)
    direct = rank < plan.slots
    piece = plan.mate(block_part) ^ plan.mate(me)
    crossed = plan.mates * plan.inner_rows + piece * plan.cross_rows
    spot = plan.spot(block_part) ^ plan.spot(me)
    relayed = plan.mates * (plan.inner_rows + plan.cross_rows) + spot * plan.relay_rows
    origin = jnp.where(home, piece * plan.inner_rows, jnp.where(direct, crossed, relayed))
    slots = jnp.where(home, plan.most, jnp.where(direct, plan.slots, 2 * plan.over))
    flip = plan.plane(block_part) ^ plan.plane(me)
    shift = jnp.where(flip == far_planes[0], 0, plan.over) - plan.slots
    slot = jnp.where(home | direct, rank, rank + shift)
    return origin + slot * plan.full, origin + slots * plan.full + slot, slots


def mixed(mates):
    pairs = [(d, mates - 1 - d) for d in range(mates // 2)]
    return [d for pair in pairs[1:] + pairs[:1] for d in pair]


def early_inner(mates, side):
    across = [d for d in mixed(mates) if d & side]
    return across[: len(across) // 2]


def exchange(plan, room, table, states, params, block_part, tile_perm):
    over = range(plan.devices)

    def send(piece, target):
        return lax.ppermute(piece, both, [(i, target(i)) for i in over])

    dense = pack_dense(plan, table, states, room)
    crossed = [
        send(piece, functools.partial(plan.twin, flip=far))
        for far, piece in zip(far_planes, dense)
    ]
    adv = advance(params, states)
    first = early_inner(plan.mates, plan.side)
    second = [d for d in range(plan.mates) if d not in first]
    inner = dict(zip(first, pack_pieces(plan, table, adv, first, [])))
    more = pack_pieces(plan, table, adv, second, list(range(plan.mates)))
    inner.update(zip(second, more))
    cross = list(more[len(second) :])
    again = list(relay(plan, table, params, crossed, room))
    for d in range(plan.mates):
        cross[d] = send(cross[d], lambda i: plan.device(plan.mate(i) ^ d, 1 - plan.half(i)))
        if d:
            inner[d] = send(inner[d], lambda i: plan.device(plan.mate(i) ^ d, plan.half(i)))
    for d in range(1, plan.flat):
        again[d] = send(again[d], lambda i: plan.at(plan.spot(i) ^ d, plan.plane(i)))
    inner = [inner[d] for d in range(plan.mates)]
    places = find_places(plan, block_part, plan.me())
    return unpack(plan, places, tile_perm, [*inner, *cross, *again])


def on_device(
    states, block_part, tile_perm, half_volt, steepness, gate_rate, conductance, reversal
):
    blocks, width = tile_perm.shape
    plan = Plan(states.shape[0], blocks, width)
    devices = plan.devices
    ids = jnp.arange(devices, dtype=jnp.int32)
    onehot = (block_part[:, None] == ids[None, :]).astype(jnp.int32)
    counts = jnp.sum(onehot, axis=0, dtype=jnp.int32)
    told = jnp.broadcast_to(counts[None, None, :], (devices, 1, devices))
    table = lax.all_to_all(told, both, split_axis=0, concat_axis=0, tiled=True)
    params = gate_params(half_volt, steepness, gate_rate, conductance, reversal, width)
    spilled = jnp.maximum(table - plan.slots, 0)
    spilled = spilled.reshape(devices // plan.peers, 4, plan.side, devices)
    spilled = jnp.sum(spilled, axis=(0, 2), dtype=jnp.int32)
    across = plan.half(ids)[None, :] != jnp.arange(4, dtype=jnp.int32)[:, None] // 2
    spilled = jnp.max(jnp.where(across, spilled, 0))
    rooms = sorted({round_up(-(-plan.worst * part // 40), 2) for part in (18, 21, 25, 40)})
    choice = sum((spilled > room).astype(jnp.int32) for room in rooms[:-1])
    return lax.switch(
        choice,
        [functools.partial(exchange, plan, room) for room in rooms],
        table,
        states,
        params,
        block_part,
        tile_perm,
    )


def solution(mesh):
    return jax.shard_map(
        on_device,
        mesh=mesh,
        in_specs=(
            P(None, both),
            P(both),
            P(both, None),
            P(),
            P(),
            P(),
            P(),
            P(),
        ),
        out_specs=P(None, both),
        check_vma=False,
    )
```

```python
import functools

import jax
import jax.numpy as jnp
from jax import lax
from jax.experimental import pallas as pl
from jax.experimental.pallas import tpu as pltpu
from jax.sharding import PartitionSpec as P


time_step = 0.25
sublanes = 8
both = ("group", "peer")
smem_full = pl.BlockSpec(memory_space=pltpu.SMEM)
vmem_full = pl.BlockSpec(memory_space=pltpu.VMEM)
any_full = pl.BlockSpec(memory_space=pl.ANY)


def round_up(value, step):
    return -(-value // step) * step


class Plan:
    def __init__(self, rows, blocks, width):
        self.rows, self.blocks, self.width = rows, blocks, width
        self.peers = lax.axis_size("peer")
        self.devices = lax.axis_size("group") * self.peers
        self.near = self.peers // 2
        self.mates = self.devices // 2
        most = 2 * blocks // self.devices
        self.slots = max(3 * most // 8, 1)
        self.over = most - self.slots
        self.full = rows // sublanes * sublanes
        self.extra = rows - self.full
        self.most = self.slots + self.over
        self.inner_rows = round_up(rows * self.most, sublanes)
        self.cross_rows = round_up(rows * self.slots, sublanes)
        self.relay_rows = round_up(rows * 2 * self.over, sublanes)
        self.side = self.peers // 4
        self.flat = self.devices // 4
        self.worst = self.flat * self.over

    def half(self, device):
        return (device % self.peers) // self.near

    def mate(self, device):
        return device // self.peers * self.near + device % self.near

    def device(self, mate, half):
        return mate // self.near * self.peers + half * self.near + mate % self.near

    def plane(self, device):
        return device % self.peers // self.side

    def spot(self, device):
        return device // self.peers * self.side + device % self.side

    def at(self, spot, plane):
        return spot // self.side * self.peers + plane * self.side + spot % self.side

    def twin(self, device, flip):
        return self.at(self.spot(device), self.plane(device) ^ flip)

    def me(self):
        return lax.axis_index("group") * self.peers + lax.axis_index("peer")


def advanced(params_ref, vals, tail):
    full = vals.shape[0]
    voltage = vals[0:1]
    relax = 1.5 + 0.5 * jnp.tanh(0.5 * voltage)
    done, current = [], 0.0
    for part, rows in ((vals, slice(0, full)), (tail, slice(full, None))):
        if part is None:
            continue
        steady = 0.5 + 0.5 * jnp.tanh((voltage - params_ref[0, rows]) * params_ref[1, rows])
        damping = jnp.exp(params_ref[2, rows] * relax)
        gates = steady + (part - steady) * damping
        drive = params_ref[3, rows] * gates * (voltage - params_ref[4, rows])
        current = current + jnp.sum(drive, axis=0, keepdims=True)
        done.append(gates)
    row = lax.broadcasted_iota(jnp.int32, vals.shape, 0)
    done[0] = jnp.where(row == 0, voltage - time_step * current, done[0])
    return done


def advance_kernel(params_ref, states_ref, out_ref, *, width):
    rows = states_ref.shape[0]
    full = rows // sublanes * sublanes

    lanes = 4 * width if states_ref.shape[1] % (4 * width) == 0 else width

    def one(i, carry):
        for j in range(lanes // width):
            at = pl.multiple_of(i * lanes + j * width, width)
            cols = pl.ds(at, width)
            tail = states_ref[full:rows, cols] if rows > full else None
            done = advanced(params_ref, states_ref[0:full, cols], tail)
            out_ref[0:full, cols] = done[0]
            if rows > full:
                out_ref[full:rows, cols] = done[1]
        return carry

    lax.fori_loop(0, states_ref.shape[1] // lanes, one, 0)


def gate_params(half_volt, steepness, gate_rate, conductance, reversal, width):
    params = jnp.stack([half_volt, 0.5 * steepness, -gate_rate, conductance, reversal])
    params = jnp.pad(params, ((0, 0), (1, 0)))
    return jnp.broadcast_to(params[:, :, None], params.shape + (width,))


def advance(params, states):
    rows, nodes = states.shape
    width = params.shape[2]
    block = fitting(nodes, 4096)
    return pl.pallas_call(
        functools.partial(advance_kernel, width=width),
        grid=(nodes // block,),
        in_specs=[
            pl.BlockSpec(params.shape, lambda i: (0, 0, 0)),
            pl.BlockSpec((rows, block), lambda i: (0, i)),
        ],
        out_specs=pl.BlockSpec((rows, block), lambda i: (0, i)),
        out_shape=jax.ShapeDtypeStruct(states.shape, states.dtype),
        cost_estimate=pl.CostEstimate(
            flops=40 * rows * nodes,
            bytes_accessed=8 * rows * nodes,
            transcendentals=3 * rows * nodes,
        ),
        name="advance",
    )(params, states)


def fitting(total, most):
    size = min(total, most)
    while total % size:
        size -= 128
    return size


def put_block(plan, adv_ref, block, put, base, tail):
    cols = pl.ds(pl.multiple_of(block * plan.width, plan.width), plan.width)
    put(base, plan.full, adv_ref[0 : plan.full, cols])
    for e in range(plan.extra):
        put(tail(e), 1, adv_ref[plan.full + e : plan.full + e + 1, cols])


far_planes = (2, 3)


def dense_kernel(table_ref, states_ref, *outs, plan, room):
    me = plan.me()

    def one(s, carry):
        start, *places = carry
        count = table_ref[s, 0, me]
        flip = plan.plane(s) ^ plan.plane(me)
        spilled = jnp.maximum(count - plan.slots, 0)
        nexts = []
        for far, at, out_ref in zip(far_planes, places, outs):
            more = spilled * (flip == far).astype(jnp.int32)

            def spill(k, carry, at=at, out_ref=out_ref):
                slot = jnp.minimum(at + k, room - 1)

                def put(base, size, vals):
                    if size == plan.full:
                        base = pl.multiple_of(base, sublanes)
                    out_ref[pl.ds(base, size), :] = vals

                put_block(
                    plan,
                    states_ref,
                    start + plan.slots + k,
                    put,
                    slot * plan.full,
                    lambda e: room * plan.full + e * room + slot,
                )
                return carry

            lax.fori_loop(0, more, spill, 0)
            nexts.append(at + more)
        return (start + count, *nexts)

    lax.fori_loop(0, plan.devices, one, (0, 0, 0))


def pack_dense(plan, table, states, room):
    rows = round_up(room * plan.rows, sublanes)
    piece = jax.ShapeDtypeStruct((rows, plan.width), states.dtype)
    return pl.pallas_call(
        functools.partial(dense_kernel, plan=plan, room=room),
        in_specs=[smem_full, vmem_full],
        out_specs=[vmem_full] * 2,
        out_shape=[piece] * 2,
        name="pack_dense",
    )(table, states)


def pieces_kernel(table_ref, adv_ref, *refs, plan, inner, cross):
    outs, start_ref = refs[:-1], refs[-1]
    me = plan.me()
    mine = plan.half(me)
    here = plan.mate(me)

    def scan(s, start):
        start_ref[s] = start
        return start + table_ref[s, 0, me]

    lax.fori_loop(0, plan.devices, scan, 0)
    jobs = [(d, mine, plan.most) for d in inner] + [(d, 1 - mine, plan.slots) for d in cross]
    for (d, half, slots), out_ref in zip(jobs, outs):
        start = start_ref[plan.device(here ^ d, half)]

        def put(base, size, vals):
            out_ref[base : base + size, :] = vals

        for k in range(slots):
            put_block(
                plan,
                adv_ref,
                jnp.minimum(start + k, plan.blocks - 1),
                put,
                k * plan.full,
                lambda e: slots * plan.full + e * slots + k,
            )


def pack_pieces(plan, table, adv, inner, cross):
    rows = [plan.inner_rows] * len(inner) + [plan.cross_rows] * len(cross)
    return pl.pallas_call(
        functools.partial(pieces_kernel, plan=plan, inner=inner, cross=cross),
        in_specs=[smem_full, vmem_full],
        out_specs=[vmem_full] * len(rows),
        out_shape=[jax.ShapeDtypeStruct((size, plan.width), adv.dtype) for size in rows],
        scratch_shapes=[pltpu.SMEM((plan.devices,), jnp.int32)],
    )(table, adv)


def relay_kernel(table_ref, params_ref, *refs, plan, room):
    dense, outs = refs[:2], refs[2 : 2 + plan.flat]
    first_refs, done_refs = refs[2 + plan.flat : 4 + plan.flat], refs[4 + plan.flat :]
    me = plan.me()
    plane = plan.plane(me)
    here = plan.spot(me)
    slots = 2 * plan.over
    for j, far in enumerate(far_planes):
        dense_ref, done_ref, first_ref = dense[j], done_refs[j], first_refs[j]
        source = plan.twin(me, far)

        def scan(t, at):
            first_ref[t] = at
            return at + jnp.maximum(table_ref[plan.at(t, plane), 0, source] - plan.slots, 0)

        total = lax.fori_loop(0, plan.flat, scan, 0)

        def step(i, carry):
            rows = pl.ds(pl.multiple_of(i * plan.full, plan.full), plan.full)
            lasts = [pl.ds(room * plan.full + e * room + i, 1) for e in range(plan.extra)]
            tail = None
            if plan.extra:
                tail = [dense_ref[last, :] for last in lasts]
                tail = jnp.concatenate(tail, axis=0) if plan.extra > 1 else tail[0]
            done = advanced(params_ref, dense_ref[rows, :], tail)
            done_ref[rows, :] = done[0]
            for e, last in enumerate(lasts):
                done_ref[last, :] = done[1][e : e + 1]
            return carry

        lax.fori_loop(0, jnp.minimum(total, room), step, 0)
        for d, out_ref in enumerate(outs):
            at = first_ref[here ^ d]
            for k in range(plan.over):
                slot = jnp.minimum(at + k, room - 1)
                to = j * plan.over + k
                out_ref[to * plan.full : (to + 1) * plan.full, :] = done_ref[
                    pl.ds(pl.multiple_of(slot * plan.full, plan.full), plan.full), :
                ]
                for e in range(plan.extra):
                    row = slots * plan.full + e * slots + to
                    out_ref[row : row + 1, :] = done_ref[
                        pl.ds(room * plan.full + e * room + slot, 1), :
                    ]


def relay(plan, table, params, dense, room):
    piece = jax.ShapeDtypeStruct((plan.relay_rows, plan.width), dense[0].dtype)
    starts = pltpu.SMEM((plan.flat,), jnp.int32)
    blocks = pltpu.VMEM(dense[0].shape, dense[0].dtype)
    return pl.pallas_call(
        functools.partial(relay_kernel, plan=plan, room=room),
        in_specs=[smem_full] + [vmem_full] * 3,
        out_specs=[vmem_full] * plan.flat,
        out_shape=[piece] * plan.flat,
        scratch_shapes=[starts, starts, blocks, blocks],
        name="relay",
    )(table, params, *dense)


def permuted(vals, lanes):
    return jnp.take_along_axis(vals, lanes, axis=1, mode="promise_in_bounds")


def unpack_kernel(base_ref, tail_ref, step_ref, perm_ref, *refs, plan, sizes):
    pieces = refs[: len(sizes)]
    out_ref, got_ref, last_ref, sem = refs[len(sizes) :]
    per_step, width = perm_ref.shape
    first = pl.program_id(0) * per_step

    @pl.when(first == 0)
    def _():
        copies, at = [], 0
        for i, (piece_ref, size) in enumerate(zip(pieces, sizes)):
            rows = pl.ds(at, size)
            copies.append(pltpu.make_async_copy(piece_ref, got_ref.at[rows], sem.at[i]))
            at += size
        for copy in copies:
            copy.start()
        for copy in copies:
            copy.wait()

    for i in range(per_step):
        base = pl.multiple_of(base_ref[first + i], sublanes)
        tail = tail_ref[first + i]
        stride = step_ref[first + i]
        lanes = jnp.broadcast_to(perm_ref[i : i + 1, :], (plan.full, width))
        vals = got_ref[pl.ds(base, plan.full), :]
        out_ref[0 : plan.full, i * width : (i + 1) * width] = permuted(vals, lanes)
        for e in range(plan.extra):
            last_ref[e, i : i + 1, :] = got_ref[pl.ds(tail + e * stride, 1), :]
    for e in range(plan.extra):
        last = permuted(last_ref[e], perm_ref[...])
        for i in range(per_step):
            cols = slice(i * width, (i + 1) * width)
            out_ref[plan.full + e : plan.full + e + 1, cols] = last[i : i + 1, :]


def unpack_early(plan, places, perm, pieces):
    per_step = fitting_blocks(plan.blocks, 16)
    sizes = [piece.shape[0] for piece in pieces]
    dtype = pieces[0].dtype
    return pl.pallas_call(
        functools.partial(unpack_kernel, plan=plan, sizes=sizes),
        grid_spec=pltpu.PrefetchScalarGridSpec(
            num_scalar_prefetch=3,
            grid=(plan.blocks // per_step,),
            in_specs=[pl.BlockSpec((per_step, plan.width), lambda i, *_: (i, 0))]
            + [any_full] * len(pieces),
            out_specs=pl.BlockSpec((plan.rows, per_step * plan.width), lambda i, *_: (0, i)),
            scratch_shapes=[
                pltpu.VMEM((sum(sizes), plan.width), dtype),
                pltpu.VMEM((max(plan.extra, 1), per_step, plan.width), dtype),
                pltpu.SemaphoreType.DMA((len(pieces),)),
            ],
        ),
        out_shape=jax.ShapeDtypeStruct((plan.rows, plan.blocks * plan.width), dtype),
        name="unpack_early",
    )(*places, perm, *pieces)


def late_kernel(
    count_ref, block_ref, base_ref, tail_ref, perm_ref, prior_ref, *refs, plan, group
):
    pieces, (out_ref, got_ref, stage_ref, last_ref, lanes_ref) = refs[:-7], refs[-7:-2]
    load_sem, store_sem = refs[-2:]
    size = plan.cross_rows
    loads = [
        pltpu.make_async_copy(piece_ref, got_ref.at[pl.ds(i * size, size)], load_sem.at[i])
        for i, piece_ref in enumerate(pieces)
    ]
    for load in loads:
        load.start()
    for load in loads:
        load.wait()
    count = count_ref[0]

    def store(i):
        cols = pl.ds(pl.multiple_of(block_ref[i] * plan.width, plan.width), plan.width)
        return pltpu.make_async_copy(
            stage_ref.at[i], out_ref.at[:, cols], store_sem.at[i]
        )

    def some(g, carry):
        for u in range(group):
            i = g * group + u
            lanes = perm_ref[pl.ds(block_ref[i], 1), :]
            lanes_ref[u : u + 1, :] = lanes
            base = pl.multiple_of(base_ref[i], sublanes)
            vals = got_ref[pl.ds(base, plan.full), :]
            wide = jnp.broadcast_to(lanes, (plan.full, plan.width))
            stage_ref[i, 0 : plan.full, :] = permuted(vals, wide)
            for e in range(plan.extra):
                row = tail_ref[i] + e * plan.slots
                last_ref[e, u : u + 1, :] = got_ref[pl.ds(row, 1), :]
        for e in range(plan.extra):
            last = permuted(last_ref[e], lanes_ref[...])
            for u in range(group):
                row = plan.full + e
                stage_ref[g * group + u, row : row + 1, :] = last[u : u + 1, :]
        for u in range(group):
            i = g * group + u

            @pl.when(i < count)
            def _(i=i):
                store(i).start()

        return carry

    lax.fori_loop(0, (count + group - 1) // group, some, 0)

    def finish(i, carry):
        store(i).wait()
        return carry

    lax.fori_loop(0, count, finish, 0)


def unpack_late(plan, late, perm, prior, pieces):
    group = sublanes
    most = round_up(plan.mates * plan.slots, group)
    dtype = prior.dtype
    return pl.pallas_call(
        functools.partial(late_kernel, plan=plan, group=group),
        grid_spec=pltpu.PrefetchScalarGridSpec(
            num_scalar_prefetch=4,
            grid=(1,),
            in_specs=[pl.BlockSpec(perm.shape, lambda i, *_: (0, 0)), any_full]
            + [any_full] * len(pieces),
            out_specs=any_full,
            scratch_shapes=[
                pltpu.VMEM((len(pieces) * plan.cross_rows, plan.width), dtype),
                pltpu.VMEM((most, plan.rows, plan.width), dtype),
                pltpu.VMEM((max(plan.extra, 1), group, plan.width), dtype),
                pltpu.VMEM((group, plan.width), perm.dtype),
                pltpu.SemaphoreType.DMA((len(pieces),)),
                pltpu.SemaphoreType.DMA((most,)),
            ],
        ),
        out_shape=jax.ShapeDtypeStruct(prior.shape, dtype),
        input_output_aliases={5: 0},
        name="unpack_late",
    )(*late, perm, prior, *pieces)


def fitting_blocks(total, most):
    size = min(total, most)
    while total % size:
        size -= 1
    return size


def find_places(plan, block_part, me):
    same = block_part[:, None] == block_part[None, :]
    position = jnp.arange(plan.blocks, dtype=jnp.int32)
    ahead = position[None, :] < position[:, None]
    rank = jnp.sum((same & ahead).astype(jnp.int32), axis=1, dtype=jnp.int32)
    home = plan.half(block_part) == plan.half(me)
    direct = rank < plan.slots
    piece = plan.mate(block_part) ^ plan.mate(me)
    spot = plan.spot(block_part) ^ plan.spot(me)
    relayed = plan.mates * plan.inner_rows + spot * plan.relay_rows
    origin = jnp.where(home, piece * plan.inner_rows, relayed)
    slots = jnp.where(home, plan.most, 2 * plan.over)
    flip = plan.plane(block_part) ^ plan.plane(me)
    shift = jnp.where(flip == far_planes[0], 0, plan.over) - plan.slots
    slot = jnp.where(home, rank, rank + shift)
    late = direct & ~home
    base = jnp.where(late, 0, origin + slot * plan.full)
    tail = jnp.where(late, 0, origin + slots * plan.full + slot)
    early = (base, tail, slots)
    order = jnp.sum((ahead & late[None, :]).astype(jnp.int32), axis=1, dtype=jnp.int32)
    chosen = late[None, :] & (order[None, :] == position[:, None])
    base = piece * plan.cross_rows + rank * plan.full
    tail = piece * plan.cross_rows + plan.slots * plan.full + rank
    count = jnp.sum(late.astype(jnp.int32), dtype=jnp.int32).reshape(1)
    listed = [
        jnp.sum(jnp.where(chosen, vals[None, :], 0), axis=1, dtype=jnp.int32)
        for vals in (position, base, tail)
    ]
    return early, (count, *listed)


def mixed(mates):
    pairs = [(d, mates - 1 - d) for d in range(mates // 2)]
    return [d for pair in pairs[1:] + pairs[:1] for d in pair]


def early_inner(mates, side):
    across = [d for d in mixed(mates) if d & side]
    return across[: len(across) // 2]


def exchange(plan, room, table, states, params, block_part, tile_perm):
    over = range(plan.devices)

    def send(piece, target):
        return lax.ppermute(piece, both, [(i, target(i)) for i in over])

    dense = pack_dense(plan, table, states, room)
    crossed = [
        send(piece, functools.partial(plan.twin, flip=far))
        for far, piece in zip(far_planes, dense)
    ]
    adv = advance(params, states)
    first = early_inner(plan.mates, plan.side)
    second = [d for d in range(plan.mates) if d not in first]
    inner = dict(zip(first, pack_pieces(plan, table, adv, first, [])))
    more = pack_pieces(plan, table, adv, second, list(range(plan.mates)))
    inner.update(zip(second, more))
    cross = list(more[len(second) :])
    again = list(relay(plan, table, params, crossed, room))
    for d in range(plan.mates):
        cross[d] = send(cross[d], lambda i: plan.device(plan.mate(i) ^ d, 1 - plan.half(i)))
        if d:
            inner[d] = send(inner[d], lambda i: plan.device(plan.mate(i) ^ d, plan.half(i)))
    for d in range(1, plan.flat):
        again[d] = send(again[d], lambda i: plan.at(plan.spot(i) ^ d, plan.plane(i)))
    inner = [inner[d] for d in range(plan.mates)]
    early, late = find_places(plan, block_part, plan.me())
    out = unpack_early(plan, early, tile_perm, [*inner, *again])
    return unpack_late(plan, late, tile_perm, out, cross)


def on_device(
    states, block_part, tile_perm, half_volt, steepness, gate_rate, conductance, reversal
):
    blocks, width = tile_perm.shape
    plan = Plan(states.shape[0], blocks, width)
    devices = plan.devices
    ids = jnp.arange(devices, dtype=jnp.int32)
    onehot = (block_part[:, None] == ids[None, :]).astype(jnp.int32)
    counts = jnp.sum(onehot, axis=0, dtype=jnp.int32)
    told = jnp.broadcast_to(counts[None, None, :], (devices, 1, devices))
    table = lax.all_to_all(told, both, split_axis=0, concat_axis=0, tiled=True)
    params = gate_params(half_volt, steepness, gate_rate, conductance, reversal, width)
    spilled = jnp.maximum(table - plan.slots, 0)
    spilled = spilled.reshape(devices // plan.peers, 4, plan.side, devices)
    spilled = jnp.sum(spilled, axis=(0, 2), dtype=jnp.int32)
    across = plan.half(ids)[None, :] != jnp.arange(4, dtype=jnp.int32)[:, None] // 2
    spilled = jnp.max(jnp.where(across, spilled, 0))
    rooms = sorted({round_up(-(-plan.worst * part // 40), 2) for part in (18, 21, 25, 40)})
    choice = sum((spilled > room).astype(jnp.int32) for room in rooms[:-1])
    return lax.switch(
        choice,
        [functools.partial(exchange, plan, room) for room in rooms],
        table,
        states,
        params,
        block_part,
        tile_perm,
    )


def solution(mesh):
    return jax.shard_map(
        on_device,
        mesh=mesh,
        in_specs=(
            P(None, both),
            P(both),
            P(both, None),
            P(),
            P(),
            P(),
            P(),
            P(),
        ),
        out_specs=P(None, both),
        check_vma=False,
    )
```

```python
import functools

import jax
import jax.numpy as jnp
from jax import lax
from jax.experimental import pallas as pl
from jax.experimental.pallas import tpu as pltpu
from jax.sharding import PartitionSpec as P


time_step = 0.25
sublanes = 8
both = ("group", "peer")
smem_full = pl.BlockSpec(memory_space=pltpu.SMEM)
vmem_full = pl.BlockSpec(memory_space=pltpu.VMEM)
any_full = pl.BlockSpec(memory_space=pl.ANY)


def round_up(value, step):
    return -(-value // step) * step


class Plan:
    def __init__(self, rows, blocks, width):
        self.rows, self.blocks, self.width = rows, blocks, width
        self.peers = lax.axis_size("peer")
        self.devices = lax.axis_size("group") * self.peers
        self.near = self.peers // 2
        self.mates = self.devices // 2
        most = 2 * blocks // self.devices
        self.slots = max(3 * most // 8, 1)
        self.over = most - self.slots
        self.full = rows // sublanes * sublanes
        self.extra = rows - self.full
        self.most = self.slots + self.over
        self.inner_rows = round_up(rows * self.most, sublanes)
        self.cross_rows = round_up(rows * self.slots, sublanes)
        self.relay_rows = round_up(rows * 2 * self.over, sublanes)
        self.side = self.peers // 4
        self.flat = self.devices // 4
        self.worst = self.flat * self.over

    def half(self, device):
        return (device % self.peers) // self.near

    def mate(self, device):
        return device // self.peers * self.near + device % self.near

    def device(self, mate, half):
        return mate // self.near * self.peers + half * self.near + mate % self.near

    def plane(self, device):
        return device % self.peers // self.side

    def spot(self, device):
        return device // self.peers * self.side + device % self.side

    def at(self, spot, plane):
        return spot // self.side * self.peers + plane * self.side + spot % self.side

    def twin(self, device, flip):
        return self.at(self.spot(device), self.plane(device) ^ flip)

    def me(self):
        return lax.axis_index("group") * self.peers + lax.axis_index("peer")


def advanced(params_ref, vals, tail):
    full = vals.shape[0]
    voltage = vals[0:1]
    relax = 1.5 + 0.5 * jnp.tanh(0.5 * voltage)
    done, current = [], 0.0
    for part, rows in ((vals, slice(0, full)), (tail, slice(full, None))):
        if part is None:
            continue
        steady = 0.5 + 0.5 * jnp.tanh((voltage - params_ref[0, rows]) * params_ref[1, rows])
        damping = jnp.exp(params_ref[2, rows] * relax)
        gates = steady + (part - steady) * damping
        drive = params_ref[3, rows] * gates * (voltage - params_ref[4, rows])
        current = current + jnp.sum(drive, axis=0, keepdims=True)
        done.append(gates)
    row = lax.broadcasted_iota(jnp.int32, vals.shape, 0)
    done[0] = jnp.where(row == 0, voltage - time_step * current, done[0])
    return done


def advance_kernel(params_ref, states_ref, out_ref, *, width):
    rows = states_ref.shape[0]
    full = rows // sublanes * sublanes

    lanes = 4 * width if states_ref.shape[1] % (4 * width) == 0 else width

    def one(i, carry):
        for j in range(lanes // width):
            at = pl.multiple_of(i * lanes + j * width, width)
            cols = pl.ds(at, width)
            tail = states_ref[full:rows, cols] if rows > full else None
            done = advanced(params_ref, states_ref[0:full, cols], tail)
            out_ref[0:full, cols] = done[0]
            if rows > full:
                out_ref[full:rows, cols] = done[1]
        return carry

    lax.fori_loop(0, states_ref.shape[1] // lanes, one, 0)


def gate_params(half_volt, steepness, gate_rate, conductance, reversal, width):
    params = jnp.stack([half_volt, 0.5 * steepness, -gate_rate, conductance, reversal])
    params = jnp.pad(params, ((0, 0), (1, 0)))
    return jnp.broadcast_to(params[:, :, None], params.shape + (width,))


def advance(params, states):
    rows, nodes = states.shape
    width = params.shape[2]
    block = fitting(nodes, 4096)
    return pl.pallas_call(
        functools.partial(advance_kernel, width=width),
        grid=(nodes // block,),
        in_specs=[
            pl.BlockSpec(params.shape, lambda i: (0, 0, 0)),
            pl.BlockSpec((rows, block), lambda i: (0, i)),
        ],
        out_specs=pl.BlockSpec((rows, block), lambda i: (0, i)),
        out_shape=jax.ShapeDtypeStruct(states.shape, states.dtype),
        cost_estimate=pl.CostEstimate(
            flops=40 * rows * nodes,
            bytes_accessed=8 * rows * nodes,
            transcendentals=3 * rows * nodes,
        ),
        name="advance",
    )(params, states)


def fitting(total, most):
    size = min(total, most)
    while total % size:
        size -= 128
    return size


def put_block(plan, adv_ref, block, put, base, tail):
    cols = pl.ds(pl.multiple_of(block * plan.width, plan.width), plan.width)
    put(base, plan.full, adv_ref[0 : plan.full, cols])
    for e in range(plan.extra):
        put(tail(e), 1, adv_ref[plan.full + e : plan.full + e + 1, cols])


far_planes = (2, 3)


def dense_kernel(table_ref, states_ref, *outs, plan, room):
    me = plan.me()

    def one(s, carry):
        start, *places = carry
        count = table_ref[s, 0, me]
        flip = plan.plane(s) ^ plan.plane(me)
        spilled = jnp.maximum(count - plan.slots, 0)
        nexts = []
        for far, at, out_ref in zip(far_planes, places, outs):
            more = spilled * (flip == far).astype(jnp.int32)

            def spill(k, carry, at=at, out_ref=out_ref):
                slot = jnp.minimum(at + k, room - 1)

                def put(base, size, vals):
                    if size == plan.full:
                        base = pl.multiple_of(base, sublanes)
                    out_ref[pl.ds(base, size), :] = vals

                put_block(
                    plan,
                    states_ref,
                    start + plan.slots + k,
                    put,
                    slot * plan.full,
                    lambda e: room * plan.full + e * room + slot,
                )
                return carry

            lax.fori_loop(0, more, spill, 0)
            nexts.append(at + more)
        return (start + count, *nexts)

    lax.fori_loop(0, plan.devices, one, (0, 0, 0))


def pack_dense(plan, table, states, room):
    rows = round_up(room * plan.rows, sublanes)
    piece = jax.ShapeDtypeStruct((rows, plan.width), states.dtype)
    return pl.pallas_call(
        functools.partial(dense_kernel, plan=plan, room=room),
        in_specs=[smem_full, vmem_full],
        out_specs=[vmem_full] * 2,
        out_shape=[piece] * 2,
        name="pack_dense",
    )(table, states)


def pieces_kernel(table_ref, adv_ref, *refs, plan, inner, cross):
    outs, start_ref = refs[:-1], refs[-1]
    me = plan.me()
    mine = plan.half(me)
    here = plan.mate(me)

    def scan(s, start):
        start_ref[s] = start
        return start + table_ref[s, 0, me]

    lax.fori_loop(0, plan.devices, scan, 0)
    jobs = [(d, mine, plan.most) for d in inner] + [(d, 1 - mine, plan.slots) for d in cross]
    for (d, half, slots), out_ref in zip(jobs, outs):
        start = start_ref[plan.device(here ^ d, half)]

        def put(base, size, vals):
            out_ref[base : base + size, :] = vals

        for k in range(slots):
            put_block(
                plan,
                adv_ref,
                jnp.minimum(start + k, plan.blocks - 1),
                put,
                k * plan.full,
                lambda e: slots * plan.full + e * slots + k,
            )


def pack_pieces(plan, table, adv, inner, cross):
    rows = [plan.inner_rows] * len(inner) + [plan.cross_rows] * len(cross)
    return pl.pallas_call(
        functools.partial(pieces_kernel, plan=plan, inner=inner, cross=cross),
        in_specs=[smem_full, vmem_full],
        out_specs=[vmem_full] * len(rows),
        out_shape=[jax.ShapeDtypeStruct((size, plan.width), adv.dtype) for size in rows],
        scratch_shapes=[pltpu.SMEM((plan.devices,), jnp.int32)],
    )(table, adv)


def relay_kernel(table_ref, params_ref, *refs, plan, room):
    dense, outs = refs[:2], refs[2 : 2 + plan.flat]
    first_refs, done_refs = refs[2 + plan.flat : 4 + plan.flat], refs[4 + plan.flat :]
    me = plan.me()
    plane = plan.plane(me)
    here = plan.spot(me)
    slots = 2 * plan.over
    for j, far in enumerate(far_planes):
        dense_ref, done_ref, first_ref = dense[j], done_refs[j], first_refs[j]
        source = plan.twin(me, far)

        def scan(t, at):
            first_ref[t] = at
            return at + jnp.maximum(table_ref[plan.at(t, plane), 0, source] - plan.slots, 0)

        total = lax.fori_loop(0, plan.flat, scan, 0)

        def step(i, carry):
            rows = pl.ds(pl.multiple_of(i * plan.full, plan.full), plan.full)
            lasts = [pl.ds(room * plan.full + e * room + i, 1) for e in range(plan.extra)]
            tail = None
            if plan.extra:
                tail = [dense_ref[last, :] for last in lasts]
                tail = jnp.concatenate(tail, axis=0) if plan.extra > 1 else tail[0]
            done = advanced(params_ref, dense_ref[rows, :], tail)
            done_ref[rows, :] = done[0]
            for e, last in enumerate(lasts):
                done_ref[last, :] = done[1][e : e + 1]
            return carry

        lax.fori_loop(0, jnp.minimum(total, room), step, 0)
        for d, out_ref in enumerate(outs):
            at = first_ref[here ^ d]
            for k in range(plan.over):
                slot = jnp.minimum(at + k, room - 1)
                to = j * plan.over + k
                out_ref[to * plan.full : (to + 1) * plan.full, :] = done_ref[
                    pl.ds(pl.multiple_of(slot * plan.full, plan.full), plan.full), :
                ]
                for e in range(plan.extra):
                    row = slots * plan.full + e * slots + to
                    out_ref[row : row + 1, :] = done_ref[
                        pl.ds(room * plan.full + e * room + slot, 1), :
                    ]


def relay(plan, table, params, dense, room):
    piece = jax.ShapeDtypeStruct((plan.relay_rows, plan.width), dense[0].dtype)
    starts = pltpu.SMEM((plan.flat,), jnp.int32)
    blocks = pltpu.VMEM(dense[0].shape, dense[0].dtype)
    return pl.pallas_call(
        functools.partial(relay_kernel, plan=plan, room=room),
        in_specs=[smem_full] + [vmem_full] * 3,
        out_specs=[vmem_full] * plan.flat,
        out_shape=[piece] * plan.flat,
        scratch_shapes=[starts, starts, blocks, blocks],
        name="relay",
    )(table, params, *dense)


def permuted(vals, lanes):
    return jnp.take_along_axis(vals, lanes, axis=1, mode="promise_in_bounds")


def unpack_kernel(base_ref, tail_ref, step_ref, perm_ref, *refs, plan, sizes):
    pieces = refs[: len(sizes)]
    out_ref, got_ref, last_ref, sem = refs[len(sizes) :]
    per_step, width = perm_ref.shape
    first = pl.program_id(0) * per_step

    @pl.when(first == 0)
    def _():
        copies, at = [], 0
        for i, (piece_ref, size) in enumerate(zip(pieces, sizes)):
            rows = pl.ds(at, size)
            copies.append(pltpu.make_async_copy(piece_ref, got_ref.at[rows], sem.at[i]))
            at += size
        for copy in copies:
            copy.start()
        for copy in copies:
            copy.wait()

    for i in range(per_step):
        base = pl.multiple_of(base_ref[first + i], sublanes)
        tail = tail_ref[first + i]
        stride = step_ref[first + i]
        lanes = jnp.broadcast_to(perm_ref[i : i + 1, :], (plan.full, width))
        vals = got_ref[pl.ds(base, plan.full), :]
        out_ref[0 : plan.full, i * width : (i + 1) * width] = permuted(vals, lanes)
        for e in range(plan.extra):
            last_ref[e, i : i + 1, :] = got_ref[pl.ds(tail + e * stride, 1), :]
    for e in range(plan.extra):
        last = permuted(last_ref[e], perm_ref[...])
        for i in range(per_step):
            cols = slice(i * width, (i + 1) * width)
            out_ref[plan.full + e : plan.full + e + 1, cols] = last[i : i + 1, :]


def unpack_early(plan, places, perm, pieces):
    per_step = fitting_blocks(plan.blocks, 16)
    sizes = [piece.shape[0] for piece in pieces]
    dtype = pieces[0].dtype
    return pl.pallas_call(
        functools.partial(unpack_kernel, plan=plan, sizes=sizes),
        grid_spec=pltpu.PrefetchScalarGridSpec(
            num_scalar_prefetch=3,
            grid=(plan.blocks // per_step,),
            in_specs=[pl.BlockSpec((per_step, plan.width), lambda i, *_: (i, 0))]
            + [any_full] * len(pieces),
            out_specs=pl.BlockSpec((plan.rows, per_step * plan.width), lambda i, *_: (0, i)),
            scratch_shapes=[
                pltpu.VMEM((sum(sizes), plan.width), dtype),
                pltpu.VMEM((max(plan.extra, 1), per_step, plan.width), dtype),
                pltpu.SemaphoreType.DMA((len(pieces),)),
            ],
        ),
        out_shape=jax.ShapeDtypeStruct((plan.rows, plan.blocks * plan.width), dtype),
        name="unpack_early",
    )(*places, perm, *pieces)


def late_kernel(
    count_ref, block_ref, base_ref, tail_ref, perm_ref, prior_ref, *refs, plan, group
):
    pieces, (out_ref, got_ref, stage_ref, last_ref, lanes_ref) = refs[:-7], refs[-7:-2]
    load_sem, store_sem = refs[-2:]
    size = plan.cross_rows
    loads = [
        pltpu.make_async_copy(piece_ref, got_ref.at[pl.ds(i * size, size)], load_sem.at[i])
        for i, piece_ref in enumerate(pieces)
    ]
    for load in loads:
        load.start()
    for load in loads:
        load.wait()
    count = count_ref[0]

    def store(i):
        cols = pl.ds(pl.multiple_of(block_ref[i] * plan.width, plan.width), plan.width)
        return pltpu.make_async_copy(
            stage_ref.at[i], out_ref.at[:, cols], store_sem.at[i]
        )

    def some(g, carry):
        for u in range(group):
            i = g * group + u
            lanes = perm_ref[pl.ds(block_ref[i], 1), :]
            lanes_ref[u : u + 1, :] = lanes
            base = pl.multiple_of(base_ref[i], sublanes)
            vals = got_ref[pl.ds(base, plan.full), :]
            wide = jnp.broadcast_to(lanes, (plan.full, plan.width))
            stage_ref[i, 0 : plan.full, :] = permuted(vals, wide)
            for e in range(plan.extra):
                row = tail_ref[i] + e * plan.slots
                last_ref[e, u : u + 1, :] = got_ref[pl.ds(row, 1), :]
        for e in range(plan.extra):
            last = permuted(last_ref[e], lanes_ref[...])
            for u in range(group):
                row = plan.full + e
                stage_ref[g * group + u, row : row + 1, :] = last[u : u + 1, :]
        for u in range(group):
            i = g * group + u

            @pl.when(i < count)
            def _(i=i):
                store(i).start()

        return carry

    lax.fori_loop(0, (count + group - 1) // group, some, 0)

    def finish(i, carry):
        store(i).wait()
        return carry

    lax.fori_loop(0, count, finish, 0)


def unpack_late(plan, late, perm, prior, pieces):
    group = sublanes
    most = round_up(plan.mates * plan.slots, group)
    dtype = prior.dtype
    return pl.pallas_call(
        functools.partial(late_kernel, plan=plan, group=group),
        grid_spec=pltpu.PrefetchScalarGridSpec(
            num_scalar_prefetch=4,
            grid=(1,),
            in_specs=[pl.BlockSpec(perm.shape, lambda i, *_: (0, 0)), any_full]
            + [any_full] * len(pieces),
            out_specs=any_full,
            scratch_shapes=[
                pltpu.VMEM((len(pieces) * plan.cross_rows, plan.width), dtype),
                pltpu.VMEM((most, plan.rows, plan.width), dtype),
                pltpu.VMEM((max(plan.extra, 1), group, plan.width), dtype),
                pltpu.VMEM((group, plan.width), perm.dtype),
                pltpu.SemaphoreType.DMA((len(pieces),)),
                pltpu.SemaphoreType.DMA((most,)),
            ],
        ),
        out_shape=jax.ShapeDtypeStruct(prior.shape, dtype),
        input_output_aliases={5: 0},
        name="unpack_late",
    )(*late, perm, prior, *pieces)


def fitting_blocks(total, most):
    size = min(total, most)
    while total % size:
        size -= 1
    return size


def find_places(plan, block_part, me):
    same = block_part[:, None] == block_part[None, :]
    position = jnp.arange(plan.blocks, dtype=jnp.int32)
    ahead = position[None, :] < position[:, None]
    rank = jnp.sum((same & ahead).astype(jnp.int32), axis=1, dtype=jnp.int32)
    home = plan.half(block_part) == plan.half(me)
    direct = rank < plan.slots
    piece = plan.mate(block_part) ^ plan.mate(me)
    spot = plan.spot(block_part) ^ plan.spot(me)
    relayed = plan.mates * plan.inner_rows + spot * plan.relay_rows
    origin = jnp.where(home, piece * plan.inner_rows, relayed)
    slots = jnp.where(home, plan.most, 2 * plan.over)
    flip = plan.plane(block_part) ^ plan.plane(me)
    shift = jnp.where(flip == far_planes[0], 0, plan.over) - plan.slots
    slot = jnp.where(home, rank, rank + shift)
    late = direct & ~home
    base = jnp.where(late, 0, origin + slot * plan.full)
    tail = jnp.where(late, 0, origin + slots * plan.full + slot)
    early = (base, tail, slots)
    order = jnp.sum((ahead & late[None, :]).astype(jnp.int32), axis=1, dtype=jnp.int32)
    chosen = late[None, :] & (order[None, :] == position[:, None])
    base = piece * plan.cross_rows + rank * plan.full
    tail = piece * plan.cross_rows + plan.slots * plan.full + rank
    count = jnp.sum(late.astype(jnp.int32), dtype=jnp.int32).reshape(1)
    listed = [
        jnp.sum(jnp.where(chosen, vals[None, :], 0), axis=1, dtype=jnp.int32)
        for vals in (position, base, tail)
    ]
    return early, (count, *listed)


def mixed(mates):
    pairs = [(d, mates - 1 - d) for d in range(mates // 2)]
    return [d for pair in pairs[1:] + pairs[:1] for d in pair]


def early_inner(mates, side):
    return [d for d in mixed(mates) if d & side]


def exchange(plan, room, table, states, params, block_part, tile_perm):
    over = range(plan.devices)

    def send(piece, target):
        return lax.ppermute(piece, both, [(i, target(i)) for i in over])

    dense = pack_dense(plan, table, states, room)
    crossed = [
        send(piece, functools.partial(plan.twin, flip=far))
        for far, piece in zip(far_planes, dense)
    ]
    adv = advance(params, states)
    first = early_inner(plan.mates, plan.side)
    second = [d for d in range(plan.mates) if d not in first]
    inner = dict(zip(first, pack_pieces(plan, table, adv, first, [])))
    more = pack_pieces(plan, table, adv, second, list(range(plan.mates)))
    inner.update(zip(second, more))
    cross = list(more[len(second) :])
    again = list(relay(plan, table, params, crossed, room))
    for d in range(plan.mates):
        cross[d] = send(cross[d], lambda i: plan.device(plan.mate(i) ^ d, 1 - plan.half(i)))
        if d:
            inner[d] = send(inner[d], lambda i: plan.device(plan.mate(i) ^ d, plan.half(i)))
    for d in range(1, plan.flat):
        again[d] = send(again[d], lambda i: plan.at(plan.spot(i) ^ d, plan.plane(i)))
    inner = [inner[d] for d in range(plan.mates)]
    early, late = find_places(plan, block_part, plan.me())
    out = unpack_early(plan, early, tile_perm, [*inner, *again])
    return unpack_late(plan, late, tile_perm, out, cross)


def on_device(
    states, block_part, tile_perm, half_volt, steepness, gate_rate, conductance, reversal
):
    blocks, width = tile_perm.shape
    plan = Plan(states.shape[0], blocks, width)
    devices = plan.devices
    ids = jnp.arange(devices, dtype=jnp.int32)
    onehot = (block_part[:, None] == ids[None, :]).astype(jnp.int32)
    counts = jnp.sum(onehot, axis=0, dtype=jnp.int32)
    told = jnp.broadcast_to(counts[None, None, :], (devices, 1, devices))
    table = lax.all_to_all(told, both, split_axis=0, concat_axis=0, tiled=True)
    params = gate_params(half_volt, steepness, gate_rate, conductance, reversal, width)
    spilled = jnp.maximum(table - plan.slots, 0)
    spilled = spilled.reshape(devices // plan.peers, 4, plan.side, devices)
    spilled = jnp.sum(spilled, axis=(0, 2), dtype=jnp.int32)
    across = plan.half(ids)[None, :] != jnp.arange(4, dtype=jnp.int32)[:, None] // 2
    spilled = jnp.max(jnp.where(across, spilled, 0))
    rooms = sorted({round_up(-(-plan.worst * part // 40), 2) for part in (17, 20, 23, 27, 40)})
    choice = sum((spilled > room).astype(jnp.int32) for room in rooms[:-1])
    return lax.switch(
        choice,
        [functools.partial(exchange, plan, room) for room in rooms],
        table,
        states,
        params,
        block_part,
        tile_perm,
    )


def solution(mesh):
    return jax.shard_map(
        on_device,
        mesh=mesh,
        in_specs=(
            P(None, both),
            P(both),
            P(both, None),
            P(),
            P(),
            P(),
            P(),
            P(),
        ),
        out_specs=P(None, both),
        check_vma=False,
    )
```
